32 devices in a mesh: pipe: 8 (over z, x), expert: 4 (over y, core).
Axes of the slice: x: 2, y: 2, z: 4, core: 2. Of those that a mesh axis runs over, the one named last changes fastest.
Arguments:
- forward_in: bfloat16 [8, 256, 3584], P('pipe', 'expert'), may hold values from -6 to 6
- forward_ids: int32 [8, 256, 1], P('pipe', 'expert'), may hold values from 0 to 1, as said below
- forward_gates: float32 [8, 256, 1], P('pipe', 'expert'), may hold values from 0.4 to 1
- grad_in: bfloat16 [8, 256, 3584], P('pipe', 'expert'), may hold values from -6 to 6
- grad_ids: int32 [8, 256, 1], P('pipe', 'expert'), may hold values from 0 to 1, as said below
- grad_gates: float32 [8, 256, 1], P('pipe', 'expert'), may hold values from 0.4 to 1
- saved_input: bfloat16 [8, 256, 3584], P('pipe', 'expert'), may hold values from -6 to 6
- saved_acts: bfloat16 [8, 4, 128, 1024], P('pipe', 'expert'), may hold values from -8 to 8
- norm_gain: float32 [8, 3584], P('pipe'), may hold values from 0.1 to 1.9
- weight_in: bfloat16 [4, 3584, 1024], P('expert'), may hold values from -0.09375 to 0.09375
- weight_out: bfloat16 [4, 512, 3584], P('expert'), may hold values from -0.1875 to 0.1875
Outputs:
- forward_out: bfloat16 [8, 256, 3584], P('pipe', 'expert')
- grad_out: bfloat16 [8, 256, 3584], P('pipe', 'expert')
The draws below stay inside these ranges and needn't reach their ends.
Inputs may be any that keep to these rules, and one draw needn't show every extreme that they name: `forward_ids`: A token's 1 ids are distinct; for each section, the 64 tokens of one device name every expert exactly 32 times. `grad_ids`: A token's 1 ids are distinct; for each section, the 64 tokens of one device name every expert exactly 32 times.
All inputs are finite; a program needn't handle non-finite values.
Results may differ from the reference program's by a relative error of at most 0.008.
Values may be sent and summed in bfloat16 or wider, within the bound.
A program may use at most 64 MiB of HBM per device.

```python
import jax
import jax.numpy as jnp
from jax import lax

D = 3584
FFW = 1024
TOP = 1
TOK_DEV = 64
SECTIONS = 8
SOURCES = 4
GROUP = 2
FF_DEV = 512
SLICES = 4
EXPERTS = 2
TOKENS = 256
CAPACITY = 32


def route_block(block_key):
    key_tokens, key_within, key_offset, key_relabel = jax.random.split(block_key, 4)
    token_order = jax.random.permutation(key_tokens, TOK_DEV)
    within_keys = jax.random.split(key_within, TOK_DEV)

    def shuffle_slots(single_key):
        return jax.random.permutation(single_key, TOP)
    within_token = jax.vmap(shuffle_slots)(within_keys)
    offset = jax.random.randint(key_offset, (), 0, EXPERTS)
    relabel = jax.random.permutation(key_relabel, EXPERTS)
    position = token_order[:, None] * TOP + within_token + offset
    return relabel[position % EXPERTS].astype(jnp.int32)


def route_table(key, salt):
    salted = jax.random.fold_in(key, salt)
    block_keys = jax.random.split(salted, SECTIONS * SOURCES)
    blocks = jax.vmap(route_block)(block_keys)
    return blocks.reshape(SECTIONS, TOKENS, TOP).astype(jnp.int32)


def draw_forward_ids(key, part):
    return route_table(key, 11)


def draw_grad_ids(key, part):
    return route_table(key, 23)


def shard_levels(stream_key, shape, cuts, least, largest):
    level, own = 1.0, jax.random.fold_in(stream_key, 6)
    for dim, shards_of in cuts:
        heights = jnp.exp(jax.random.uniform(jax.random.fold_in(own, dim), (shards_of,), jnp.float32, least / len(cuts), largest / len(cuts)))
        level = level * jnp.repeat(heights, shape[dim] // shards_of).reshape([-1 if axis == dim else 1 for axis in range(len(shape))])
    return level


def bell_draw(stream_key, dims, scale, most, cuts=(), dtype=jnp.bfloat16):
    level = shard_levels(stream_key, dims, cuts, -0.22, 0.18) if cuts else 1.0
    values = jax.random.normal(stream_key, dims, jnp.float32) * scale * level
    return jnp.minimum(jnp.maximum(values, -most), most).astype(dtype)


def setup_inputs(seed: int = 0) -> dict:
    arg_keys = jax.random.split(jax.random.key(seed), 12)
    return {
        "forward_in": bell_draw(arg_keys[0], (SECTIONS, TOKENS, D), 1.0, 6.0, ((0, 8), (1, 4))),
        "forward_ids": draw_forward_ids(jax.random.fold_in(arg_keys[11], 71), 0),
        "forward_gates": jnp.clip(0.4 + 0.6 * jax.random.uniform(arg_keys[2], (SECTIONS, TOKENS, TOP), jnp.float32) ** shard_levels(arg_keys[2], (SECTIONS, TOKENS, TOP), ((0, 8), (1, 4)), -0.2, 0.2), 0.4, 1.0),
        "grad_in": bell_draw(arg_keys[3], (SECTIONS, TOKENS, D), 1.0, 6.0, ((0, 8), (1, 4))),
        "grad_ids": draw_grad_ids(jax.random.fold_in(arg_keys[11], 71), 0),
        "grad_gates": jnp.clip(0.4 + 0.6 * jax.random.uniform(arg_keys[5], (SECTIONS, TOKENS, TOP), jnp.float32) ** shard_levels(arg_keys[5], (SECTIONS, TOKENS, TOP), ((0, 8), (1, 4)), -0.2, 0.2), 0.4, 1.0),
        "saved_input": bell_draw(arg_keys[6], (SECTIONS, TOKENS, D), 1.0, 6.0, ((0, 8), (1, 4))),
        "saved_acts": bell_draw(arg_keys[7], (SECTIONS, SLICES, SOURCES * CAPACITY, 2 * FF_DEV), 1.5, 8.0, ((0, 8), (1, 4))),
        "norm_gain": jnp.clip(1.0 + 0.18 * jax.random.normal(arg_keys[8], (SECTIONS, D), jnp.float32), 0.1, 1.9),
        "weight_in": bell_draw(arg_keys[9], (SLICES, D, 2 * FF_DEV), D ** -0.5, 0.09375, ((0, 4),)),
        "weight_out": bell_draw(arg_keys[10], (SLICES, FF_DEV, D), FFW ** -0.5, 0.1875, ((0, 4),)),
    }


epsilon = 1e-06

def normalize(tokens, norm_scale):
    widened = tokens.astype(jnp.float32)
    inverse_rms = lax.rsqrt(lax.optimization_barrier(jnp.mean(widened * widened, axis=-1, keepdims=True)) + epsilon)
    return (widened * inverse_rms * norm_scale).astype(jnp.bfloat16)

def slot_order(route_ids):
    flattened = route_ids.reshape(-1)
    sorted_pairs = jnp.argsort(flattened, stable=True).astype(jnp.int32)
    inverse_pairs = jnp.argsort(sorted_pairs, stable=True).astype(jnp.int32)
    return (sorted_pairs, inverse_pairs)

def reference(forward_in, forward_ids, forward_gates, grad_in, grad_ids, grad_gates, saved_input, saved_acts, norm_gain, weight_in, weight_out):
    w_first = weight_in.astype(jnp.float32).reshape(EXPERTS, GROUP, D, 2 * FF_DEV)
    w_second = weight_out.astype(jnp.float32).reshape(EXPERTS, GROUP, FF_DEV, D)

    def section_forward(operands):
        tokens, route_ids, gate_values, norm_scale = operands
        normed = normalize(tokens, norm_scale)
        sorted_pairs, inverse_pairs = slot_order(route_ids)
        grouped = jnp.take(normed, sorted_pairs // TOP, axis=0).reshape(EXPERTS, -1, D).astype(jnp.float32)
        projected = jnp.einsum('erd,egdf->egrf', grouped, w_first)
        hidden = (jax.nn.silu(projected[..., :FF_DEV]) * projected[..., FF_DEV:]).astype(jnp.bfloat16)
        parts = jnp.einsum('egrf,egfd->egrd', hidden.astype(jnp.float32), w_second).astype(jnp.bfloat16)
        pair_out = lax.optimization_barrier(jnp.sum(parts.astype(jnp.float32), axis=1)).reshape(-1, D)
        paired = jnp.take(pair_out, inverse_pairs, axis=0).reshape(-1, TOP, D)
        combined = jnp.einsum('tk,tkd->td', gate_values, paired)
        return (tokens.astype(jnp.float32) + combined).astype(jnp.bfloat16)

    def section_backward(operands):
        grads, route_ids, gate_values, before, stored, norm_scale = operands
        sorted_pairs, inverse_pairs = slot_order(route_ids)
        grouped = jnp.take(grads, sorted_pairs // TOP, axis=0).reshape(EXPERTS, -1, D).astype(jnp.float32)
        stored_wide = stored.astype(jnp.float32).reshape(EXPERTS, GROUP, -1, 2 * FF_DEV)
        hidden_grad = jnp.einsum('erd,egfd->egrf', grouped, w_second)
        gate_act = stored_wide[..., :FF_DEV]
        up_act = stored_wide[..., FF_DEV:]
        squashed = jax.nn.sigmoid(gate_act)
        gate_grad = (hidden_grad * up_act * squashed * (1.0 + gate_act * (1.0 - squashed))).astype(jnp.bfloat16)
        up_grad = (hidden_grad * gate_act * squashed).astype(jnp.bfloat16)
        joined = jnp.concatenate([gate_grad, up_grad], axis=-1).astype(jnp.float32)
        parts = jnp.einsum('egrf,egdf->egrd', joined, w_first).astype(jnp.bfloat16)
        pair_back = lax.optimization_barrier(jnp.sum(parts.astype(jnp.float32), axis=1)).reshape(-1, D)
        paired = jnp.take(pair_back, inverse_pairs, axis=0).reshape(-1, TOP, D)
        pulled = jnp.einsum('tk,tkd->td', gate_values, paired)
        widened = before.astype(jnp.float32)
        inverse_rms = lax.rsqrt(lax.optimization_barrier(jnp.mean(widened * widened, axis=-1, keepdims=True)) + epsilon)
        unit_rows = widened * inverse_rms
        weighted = pulled * norm_scale
        through = grads.astype(jnp.float32) + inverse_rms * (weighted - unit_rows * lax.optimization_barrier(jnp.mean(weighted * unit_rows, axis=-1, keepdims=True)))
        return through.astype(jnp.bfloat16)
    moved = lax.map(section_forward, (forward_in, forward_ids, forward_gates, norm_gain))
    through = lax.map(section_backward, (grad_in, grad_ids, grad_gates, saved_input, saved_acts, norm_gain))
    return (jnp.roll(moved, 1, axis=0), jnp.roll(through, -1, axis=0))
```

```python
import functools

import jax
import jax.numpy as jnp
from jax import lax
from jax.experimental import pallas as pl
from jax.experimental.pallas import tpu as pltpu
from jax.sharding import PartitionSpec as P

epsilon = 1e-06
F32 = jnp.float32
BF16 = jnp.bfloat16
MESH = pl.DeviceIdType.MESH


def tile_of(width, most):
    tile = most
    while width % tile:
        tile //= 2
    return tile


def dot(a, b):
    return lax.dot_general(a, b, (((1,), (0,)), ((), ())), preferred_element_type=F32)


def dot_t(a, b):
    return lax.dot_general(a, b, (((1,), (1,)), ((), ())), preferred_element_type=F32)


def placing(ids_row, own, experts, capacity, padded):
    count = ids_row.shape[1]
    down = lax.broadcasted_iota(jnp.int32, (count, count), 0)
    across = lax.broadcasted_iota(jnp.int32, (count, count), 1)
    rel = ids_row - own
    rel = jnp.where(rel < 0, rel + experts, rel).astype(F32)
    spread = jnp.broadcast_to(rel, (count, count))
    column = jnp.sum(jnp.where(down == across, spread, 0.0), axis=1, keepdims=True)
    before = jnp.where((column == spread) & (down < across), 1.0, 0.0)
    rank = jnp.sum(before, axis=0, keepdims=True)
    slot = jnp.broadcast_to(rel * capacity + rank, (count, count))
    slot_column = jnp.sum(jnp.where(down == across, slot, 0.0), axis=1, keepdims=True)
    gather = jnp.where(down.astype(F32) == slot, 1.0, 0.0)
    wide = lax.broadcasted_iota(jnp.int32, (count, padded), 1).astype(F32)
    scatter = jnp.where(slot_column == wide, 1.0, 0.0).astype(BF16)
    return gather, scatter


def kernel(
    dims,
    fid_hbm, fgate_hbm, gid_hbm, ggate_hbm, gain_hbm,
    x_hbm, g_hbm, saved_hbm, acts_hbm, wi_hbm, wo_hbm,
    fin_f, fin_b, ur_f, ur_b,
    fid_ref, fgate_ref, gid_ref, ggate_ref, gain_ref,
    x_ref, g_ref, saved_ref, acts_ref, wi, wo, gain_f,
    xs_f, xs_b, rx_f, rx_b, gs_f, rg_f, us_f, us_b,
    part_f, part_b, rpart_f, rpart_b, own_f, own_b,
    mv, pb, ret_b, th, srt, hidden_ref, joined,
    w_sem, ready_sem,
    disp_s, disp_r, gate_s, gate_r, relay_s, relay_r, perm_s, perm_r, red_s, red_r,
    move_s, move_r, out_s, out_r, ret_s, ret_r,
):
    pipes, E, G = dims
    s = lax.axis_index("pipe")
    position = lax.axis_index("expert")
    e = position // G
    g = position % G
    C, D = xs_f.shape[1:]
    T = x_ref.shape[0]
    F = wo.shape[0]

    def dev(hop, k, j):
        return (
            (s + hop + pipes) % pipes,
            ((e + k + E) % E) * G + (g + j + G) % G,
        )

    near = [dev(0, k, 0) for k in range(1, E)] + [dev(0, 0, j) for j in range(1, G)]
    following = [dev(1, k, 0) for k in range(E)]
    previous = [dev(-1, k, 0) for k in range(E)]
    first, last = s == 0, s == pipes - 1

    def greet(sem, peers):
        for peer in peers:
            pl.semaphore_signal(sem, inc=1, device_id=peer, device_id_type=MESH)

    barrier = pltpu.get_barrier_semaphore()
    greet(barrier, near)
    greet(barrier, previous)
    pl.when(s != pipes - 1)(lambda: greet(barrier, following))
    pairs = (
        (gid_hbm, gid_ref), (g_hbm, g_ref), (fid_hbm, fid_ref), (fgate_hbm, fgate_ref),
        (ggate_hbm, ggate_ref), (gain_hbm, gain_ref), (x_hbm, x_ref), (saved_hbm, saved_ref), (acts_hbm, acts_ref),
        (wo_hbm, wo), (wi_hbm, wi),
    )
    loads = [
        pltpu.make_async_copy(source, held, w_sem.at[i]) for i, (source, held) in enumerate(pairs)
    ]
    for load in loads:
        load.start()
    load_gid, load_g, *load_small, load_x, load_saved, load_acts, load_wo, load_wi = loads

    started = []

    def remote(src, dst, send, recv, target):
        copy = pltpu.make_async_remote_copy(
            src_ref=src, dst_ref=dst, send_sem=send, recv_sem=recv,
            device_id=target, device_id_type=MESH,
        )
        copy.start()
        started.append(copy)
        return copy

    xs, rx = (xs_f, xs_b), (rx_f, rx_b)
    part, rpart = (part_f, part_b), (rpart_f, rpart_b)
    own = (own_f, own_b)
    halves = 2 if C % 32 == 0 else 1
    half = C // halves

    with jax.named_scope("w_gid"):
        load_gid.wait()
    gather_b, scatter_b = placing(gid_ref[...], e, E, C, us_b.shape[1])
    gather_b_rows = gather_b.astype(BF16)
    with jax.named_scope("w_bar"):
        pl.semaphore_wait(barrier, len(near) + E * (1 + (s + pipes - 1) // pipes))
    pl.when(last)(lambda: greet(ready_sem, following))
    with jax.named_scope("w_g"):
        load_g.wait()
    xs_b[...] = dot(gather_b_rows, g_ref[...]).reshape(E, C, D).astype(BF16)


    disp, gate_copy, relay = {}, {}, {}
    for k in range(1, E):
        disp[1, k] = remote(
            xs_b.at[k], rx_b.at[k, 0], disp_s.at[1, k], disp_r.at[1, k], dev(0, k, 0)
        )
    for j in range(1, G):
        relay[1, 0, j] = remote(
            xs_b.at[0], rx_b.at[0, j], relay_s.at[1, 0, j], relay_r.at[1, 0, j], dev(0, 0, j)
        )
    for load in load_small:
        load.wait()
    gather_f, scatter_f = placing(fid_ref[...], e, E, C, us_f.shape[1])
    with jax.named_scope("w_x"):
        load_x.wait()
    xs_f[...] = dot(gather_f.astype(BF16), x_ref[...]).reshape(E, C, D).astype(BF16)
    for k in range(E):
        disp[0, k] = remote(
            xs_f.at[k], rx_f.at[k, 0], disp_s.at[0, k], disp_r.at[0, k], dev(1, k, 0)
        )
    us_b[...] = scatter_b
    us_f[...] = scatter_f
    gates_b = jnp.sum(gather_b * ggate_ref[...], axis=1, keepdims=True)
    gates_f = jnp.sum(gather_f * fgate_ref[...], axis=1, keepdims=True)
    gs_f[...] = jnp.broadcast_to(gates_f, (T, gs_f.shape[2])).reshape(gs_f.shape)
    gain_copy = remote(gain_ref, gain_f, perm_s.at[2], perm_r.at[2], dev(1, 0, 0))
    for k in range(E):
        gate_copy[k] = remote(gs_f.at[k], rg_f.at[k], gate_s.at[k], gate_r.at[k], dev(1, k, 0))
    perm_f = remote(us_f, ur_f, perm_s.at[0], perm_r.at[0], dev(1, 0, 0))

    rx_b[0, 0] = xs_b[0]
    with jax.named_scope("w_saved"):
        load_saved.wait()
    srt[...] = dot(gather_b_rows, saved_ref[...]).reshape(E, C, D).astype(BF16)

    def pass_on(b, k):
        disp[b, k].wait_recv()
        for j in range(1, G):
            relay[b, k, j] = remote(
                rx[b].at[k, 0], rx[b].at[k, j], relay_s.at[b, k, j], relay_r.at[b, k, j],
                dev(0, 0, j),
            )

    def arrived(b, k):
        for j in range(1, G):
            relay[b, k, j].wait_recv()

    tile_f = tile_of(F, 256)
    tile_d = tile_of(D, 512)
    reduce = {}

    def put_part(b, k, rows, columns):
        rows = rows.reshape(G, C, tile_d)
        own[b][k, :, columns] = rows[0]
        for j in range(1, G):
            part[b][k, j, :, columns] = rows[G - j].astype(BF16)

    def send_part(b, k):
        for j in range(1, G):
            reduce[b, k, j] = remote(
                part[b].at[k, j], rpart[b].at[k, j], red_s.at[b, k, j], red_r.at[b, k, j],
                dev(0, 0, j),
            )

    def summed(b, k):
        total = own[b][k]
        for j in range(1, G):
            reduce[b, k, j].wait_recv()
            total = total + rpart[b][k, j].astype(F32)
        return total

    def forward_first():
        for k in range(E):
            arrived(0, k)
        rows = rx_f[...].astype(F32).reshape(E * G * C, D)
        inverse = lax.rsqrt(jnp.mean(rows * rows, axis=-1, keepdims=True) + epsilon)
        normed = (rows * inverse * gain_f[...]).astype(BF16)
        for f in range(0, F, tile_f):
            gate = dot(normed, wi[:, f : f + tile_f])
            up = dot(normed, wi[:, F + f : F + f + tile_f])
            hidden_ref[:, f : f + tile_f] = (jax.nn.silu(gate) * up).astype(BF16)

    def forward_second():
        hidden = hidden_ref[...]

        for d in range(0, D, tile_d):
            columns = slice(d, d + tile_d)
            rows = dot(hidden, wo[:, columns]).reshape(E, G, C, tile_d)
            for k in range(E):
                put_part(0, k, rows[k], columns)
        for k in reversed(range(E)):
            send_part(0, k)

    def forward_end(k):
        total = summed(0, k)
        gate_copy[k].wait_recv()
        moved = (rx_f[k, 0].astype(F32) + rg_f[k][:, :1] * total).astype(BF16)
        if k == 0:
            fin_f[0] = moved
            return
        mv[k] = moved
        ends.append(
            remote(mv.at[k], fin_f.at[k], move_s.at[k], move_r.at[k], dev(0, -k, 0))
        )

    def backward_first(k):
        arrived(1, k)
        rows = rx_b[k].astype(F32).reshape(G * C, D).astype(BF16)
        acts = []
        for j in range(G):
            source = ((e - k + E) % E) * G + (g - j + G) % G
            acts.append(acts_ref[source].astype(F32))
        acts = jnp.concatenate(acts, axis=0)
        for f in range(0, F, tile_f):
            grad = dot_t(rows, wo[f : f + tile_f, :])
            gate_act = acts[:, f : f + tile_f]
            up_act = acts[:, F + f : F + f + tile_f]
            squashed = jax.nn.sigmoid(gate_act)
            joined[:, f : f + tile_f] = (
                grad * up_act * squashed * (1.0 + gate_act * (1.0 - squashed))
            ).astype(BF16)
            joined[:, F + f : F + f + tile_f] = (grad * gate_act * squashed).astype(BF16)

    def backward_second(k):
        both = joined[...]

        for d in range(0, D, tile_d):
            columns = slice(d, d + tile_d)
            put_part(1, k, dot_t(both, wi[columns, :]), columns)
        send_part(1, k)

    back = {}

    def backward_return(k):
        pb[k] = summed(1, k).astype(BF16)
        for h in range(halves):
            rows = pl.ds(h * half, half)
            back[k, h] = remote(
                pb.at[k, rows], ret_b.at[k, rows], ret_s.at[k, h], ret_r.at[k, h], dev(0, -k, 0)
            )

    def backward_end(k, h):
        low, high = h * half, (h + 1) * half
        if k:
            back[k, h].wait_recv()
            pulled = ret_b[k, low:high].astype(F32)
        else:
            pulled = own_b[0, low:high]
            for j in range(1, G):
                if h == 0:
                    reduce[1, 0, j].wait_recv()
                pulled = pulled + rpart_b[0, j, low:high].astype(F32)
        weighted = gates_b[k * C + low : k * C + high] * pulled * gain_ref[...]
        before = srt[k, low:high].astype(F32)
        inverse = lax.rsqrt(jnp.mean(before * before, axis=-1, keepdims=True) + epsilon)
        unit = before * inverse
        inner = jnp.mean(weighted * unit, axis=-1, keepdims=True)
        th[k, low:high] = (
            xs_b[k, low:high].astype(F32) + inverse * (weighted - unit * inner)
        ).astype(BF16)
        rows = pl.ds(low, half)
        ends.append(
            remote(
                th.at[k, rows], fin_b.at[k, rows], out_s.at[k, h], out_r.at[k, h], dev(-1, 0, 0)
            )
        )

    ends = []
    with jax.named_scope("w_wo"):
        load_wo.wait()
    load_acts.wait()
    with jax.named_scope("b1_0"):
        backward_first(0)
    with jax.named_scope("w_wi"):
        load_wi.wait()
    with jax.named_scope("b2_0"):
        backward_second(0)
    for k in range(1, E):
        with jax.named_scope("pass1"):
            pass_on(1, k)
    with jax.named_scope("w_prev"):
        pl.when(first)(lambda: pl.semaphore_wait(ready_sem, E))
    perm_b = remote(us_b, ur_b, perm_s.at[1], perm_r.at[1], dev(-1, 0, 0))
    for h in range(halves):
        with jax.named_scope("bend0"):
            backward_end(0, h)
    for k in range(1, E):
        with jax.named_scope("b1_1"):
            backward_first(k)
        with jax.named_scope("b2_1"):
            backward_second(k)
    for k in range(1, E):
        with jax.named_scope("bret"):
            backward_return(k)
    for k in range(E):
        with jax.named_scope("pass0"):
            pass_on(0, k)
    with jax.named_scope("w_gain"):
        gain_copy.wait_recv()
    with jax.named_scope("f1"):
        forward_first()
    with jax.named_scope("f2"):
        forward_second()
    for k in range(1, E):
        with jax.named_scope("fend1"):
            forward_end(k)
    for k in range(1, E):
        for h in range(halves):
            with jax.named_scope("bend1"):
                backward_end(k, h)
    with jax.named_scope("fend0"):
        forward_end(0)

    with jax.named_scope("w_perm0"):
        perm_f.wait_recv()
    with jax.named_scope("w_perm1"):
        perm_b.wait_recv()
    for copy in ends:
        with jax.named_scope("w_end"):
            copy.wait_recv()
    with jax.named_scope("w_sends"):
        for copy in started:
            copy.wait_send()


UNSORT_STEPS = 2


def unsort(fin_f, fin_b, ur_f, ur_b, fout_hbm, gout_hbm, held, sems):
    T, D = fout_hbm.shape
    width = D // UNSORT_STEPS
    copies = []
    for i, (fin, ur, out) in enumerate(((fin_f, ur_f, fout_hbm), (fin_b, ur_b, gout_hbm))):
        for c in range(UNSORT_STEPS):
            columns = pl.ds(c * width, width)
            rows = fin[:, :, columns].astype(F32).reshape(T, width).astype(BF16)
            held[i, :, columns] = dot(ur[:, :T], rows).astype(BF16)
            copy = pltpu.make_async_copy(held.at[i, :, columns], out.at[:, columns], sems.at[i, c])
            copy.start()
            copies.append(copy)
    for copy in copies:
        copy.wait()


def on_device(
    dims,
    forward_in,
    forward_ids,
    forward_gates,
    grad_in,
    grad_ids,
    grad_gates,
    saved_input,
    saved_acts,
    norm_gain,
    weight_in,
    weight_out,
):
    pipes, E, G = dims
    T, D = forward_in.shape[1:]
    F = weight_out.shape[1]
    C = T // E
    padded = -(-T // 128) * 128
    DMA = pltpu.SemaphoreType.DMA
    rows = (E, C, D)
    vmem = pl.BlockSpec(memory_space=pltpu.VMEM)
    hbm = pl.BlockSpec(memory_space=pl.ANY)
    sorted_rows = jax.ShapeDtypeStruct(rows, BF16)
    order = jax.ShapeDtypeStruct((T, padded), BF16)
    halves = 2 if C % 32 == 0 else 1
    arrived = pl.pallas_call(
        functools.partial(kernel, dims),
        out_shape=(pltpu.VMEM(rows, BF16), pltpu.VMEM(rows, BF16), pltpu.VMEM((T, padded), BF16), pltpu.VMEM((T, padded), BF16)),
        in_specs=[hbm] * 11,
        out_specs=(vmem, vmem, vmem, vmem),
        scratch_shapes=[
            pltpu.VMEM((1, T), jnp.int32), pltpu.VMEM((1, T), F32),
            pltpu.VMEM((1, T), jnp.int32), pltpu.VMEM((1, T), F32),
            pltpu.VMEM((1, D), F32),
            pltpu.VMEM((T, D), BF16), pltpu.VMEM((T, D), BF16), pltpu.VMEM((T, D), BF16),
            pltpu.VMEM((E * G, C, 2 * F), BF16),
            pltpu.VMEM((D, 2 * F), BF16),
            pltpu.VMEM((F, D), BF16),
            pltpu.VMEM((1, D), F32),
            pltpu.VMEM(rows, BF16), pltpu.VMEM(rows, BF16),
            pltpu.VMEM((E, G, C, D), BF16), pltpu.VMEM((E, G, C, D), BF16),
            pltpu.VMEM((E, C, 128), F32), pltpu.VMEM((E, C, 128), F32),
            pltpu.VMEM((T, padded), BF16), pltpu.VMEM((T, padded), BF16),
            pltpu.VMEM((E, G, C, D), BF16), pltpu.VMEM((E, G, C, D), BF16),
            pltpu.VMEM((E, G, C, D), BF16), pltpu.VMEM((E, G, C, D), BF16),
            pltpu.VMEM(rows, F32), pltpu.VMEM(rows, F32),
            pltpu.VMEM(rows, BF16), pltpu.VMEM(rows, BF16), pltpu.VMEM(rows, BF16),
            pltpu.VMEM(rows, BF16), pltpu.VMEM(rows, BF16),
            pltpu.VMEM((E * G * C, F), BF16),
            pltpu.VMEM((G * C, 2 * F), BF16),
            DMA((11,)), pltpu.SemaphoreType.REGULAR,
            DMA((2, E)), DMA((2, E)), DMA((E,)), DMA((E,)),
            DMA((2, E, G)), DMA((2, E, G)), DMA((3,)), DMA((3,)),
            DMA((2, E, G)), DMA((2, E, G)), DMA((E,)), DMA((E,)),
            DMA((E, halves)), DMA((E, halves)), DMA((E, halves)), DMA((E, halves)),
        ],
        compiler_params=pltpu.CompilerParams(
            collective_id=0, has_side_effects=True, vmem_limit_bytes=40 * 2**20
        ),
    )(*[
        pltpu.with_memory_space_constraint(a, pltpu.HBM)
        for a in (
            forward_ids.reshape(1, T),
            forward_gates.reshape(1, T),
            grad_ids.reshape(1, T),
            grad_gates.reshape(1, T),
            norm_gain,
            forward_in[0],
            grad_in[0],
            saved_input[0],
            saved_acts.reshape(E * G, C, 2 * F),
            weight_in[0],
            weight_out[0],
        )
    ])
    out_shape = jax.ShapeDtypeStruct((T, D), BF16)
    fwd, grad = pl.pallas_call(
        unsort,
        out_shape=(out_shape, out_shape),
        in_specs=[vmem] * 4,
        out_specs=(hbm, hbm),
        scratch_shapes=[pltpu.VMEM((2, T, D), BF16), DMA((2, UNSORT_STEPS))],
        compiler_params=pltpu.CompilerParams(vmem_limit_bytes=8 * 2**20),
    )(*[pltpu.with_memory_space_constraint(a, pltpu.VMEM) for a in arrived])
    return fwd[None], grad[None]


def solution(mesh):
    sources = mesh.shape["expert"]
    G = min(4, sources // 2)
    dims = (mesh.shape["pipe"], sources // G, G)
    placed = (
        P("pipe", "expert", None),
        P("pipe", "expert", None),
        P("pipe", "expert", None),
        P("pipe", "expert", None),
        P("pipe", "expert", None),
        P("pipe", "expert", None),
        P("pipe", "expert", None),
        P("pipe", "expert", None, None),
        P("pipe", None),
        P("expert", None, None),
        P("expert", None, None),
    )
    return jax.shard_map(
        functools.partial(on_device, dims),
        mesh=mesh,
        in_specs=placed,
        out_specs=(P("pipe", "expert", None), P("pipe", "expert", None)),
        check_vma=False,
    )
```

```python
import functools

import jax
import jax.numpy as jnp
from jax import lax
from jax.experimental import pallas as pl
from jax.experimental.pallas import tpu as pltpu
from jax.sharding import PartitionSpec as P

epsilon = 1e-06
F32 = jnp.float32
BF16 = jnp.bfloat16
MESH = pl.DeviceIdType.MESH


def tile_of(width, most):
    tile = most
    while width % tile:
        tile //= 2
    return tile


LAG = 2


def disp_rows(C):
    return 2 if C % 32 == 0 else 1


def columns_of(D, C):
    tile = tile_of(D, 512)
    tiles = D // tile
    width = tile * (-(-tiles // 4) if C % 32 == 0 else tiles)
    return [slice(d, min(d + width, D)) for d in range(0, D, width)]


def dot(a, b):
    return lax.dot_general(a, b, (((1,), (0,)), ((), ())), preferred_element_type=F32)


def dot_t(a, b):
    return lax.dot_general(a, b, (((1,), (1,)), ((), ())), preferred_element_type=F32)


def placing(ids_row, own, experts, capacity, padded):
    count = ids_row.shape[1]
    down = lax.broadcasted_iota(jnp.int32, (count, count), 0)
    across = lax.broadcasted_iota(jnp.int32, (count, count), 1)
    rel = ids_row - own
    rel = jnp.where(rel < 0, rel + experts, rel).astype(F32)
    spread = jnp.broadcast_to(rel, (count, count))
    column = jnp.sum(jnp.where(down == across, spread, 0.0), axis=1, keepdims=True)
    before = jnp.where((column == spread) & (down < across), 1.0, 0.0)
    rank = jnp.sum(before, axis=0, keepdims=True)
    slot = jnp.broadcast_to(rel * capacity + rank, (count, count))
    slot_column = jnp.sum(jnp.where(down == across, slot, 0.0), axis=1, keepdims=True)
    gather = jnp.where(down.astype(F32) == slot, 1.0, 0.0)
    wide = lax.broadcasted_iota(jnp.int32, (count, padded), 1).astype(F32)
    scatter = jnp.where(slot_column == wide, 1.0, 0.0).astype(BF16)
    return gather, scatter


def kernel(
    dims,
    fid_hbm, fgate_hbm, gid_hbm, ggate_hbm, gain_hbm,
    x_hbm, g_hbm, saved_hbm, acts_hbm, wi_hbm, wo_hbm,
    fin_f, fin_b, ur_f, ur_b,
    fid_ref, fgate_ref, gid_ref, ggate_ref, gain_ref,
    x_ref, g_ref, saved_ref, acts_ref, wi, wo, gain_f,
    xs_f, xs_b, rx_f, rx_b, gs_f, rg_f, us_f, us_b,
    part_f, part_b, rpart_f, rpart_b, own_f, own_b,
    mv, pb, ret_b, th, srt, hidden_ref, joined, sum_b, both_b, sum_f, square_f,
    via, w_sem, ready_sem, via_s, via_r,
    disp_s, disp_r, gate_s, gate_r, relay_s, relay_r, perm_s, perm_r, red_s, red_r, near_r,
    move_s, move_r, out_s, out_r, ret_s, ret_r,
):
    pipes, E, G = dims
    s = lax.axis_index("pipe")
    position = lax.axis_index("expert")
    e = position // G
    g = position % G
    C, D = xs_f.shape[1:]
    T = x_ref.shape[0]
    F = wo.shape[0]

    def dev(hop, k, j):
        return (
            (s + hop + pipes) % pipes,
            ((e + k + E) % E) * G + (g + j + G) % G,
        )

    near = [dev(0, k, 0) for k in range(1, E)] + [dev(0, 0, j) for j in range(1, G)]
    following = [dev(1, k, 0) for k in range(E)]
    previous = [dev(-1, k, 0) for k in range(E)]
    first, last = s == 0, s == pipes - 1

    def greet(sem, peers):
        for peer in peers:
            pl.semaphore_signal(sem, inc=1, device_id=peer, device_id_type=MESH)

    barrier = pltpu.get_barrier_semaphore()
    greet(barrier, near)
    greet(barrier, previous)
    pl.when(s != pipes - 1)(lambda: greet(barrier, following))
    pairs = (
        (gid_hbm, gid_ref), (g_hbm, g_ref), (fid_hbm, fid_ref), (fgate_hbm, fgate_ref),
        (ggate_hbm, ggate_ref), (gain_hbm, gain_ref), (x_hbm, x_ref), (saved_hbm, saved_ref), (acts_hbm, acts_ref),
        (wo_hbm, wo), (wi_hbm, wi),
    )
    loads = [
        pltpu.make_async_copy(source, held, w_sem.at[i]) for i, (source, held) in enumerate(pairs)
    ]
    for load in loads:
        load.start()
    load_gid, load_g, *load_small, load_x, load_saved, load_acts, load_wo, load_wi = loads

    def remote(src, dst, send, recv, target):
        copy = pltpu.make_async_remote_copy(
            src_ref=src, dst_ref=dst, send_sem=send, recv_sem=recv,
            device_id=target, device_id_type=MESH,
        )
        copy.start()
        return copy

    def whole(src, dst, send, recv, target=None):
        return pltpu.make_async_remote_copy(
            src_ref=src, dst_ref=dst, send_sem=send, recv_sem=recv,
            device_id=dev(1, 0, 0) if target is None else target, device_id_type=MESH,
        )

    xs, rx = (xs_f, xs_b), (rx_f, rx_b)
    part, rpart = (part_f, part_b), (rpart_f, rpart_b)
    own = (own_f, own_b)
    halves = disp_rows(C)
    half = C // halves
    tile_d = tile_of(D, 512)
    chunks = columns_of(D, C)
    count = len(chunks)
    others = range(1, E)

    def flat(rows):
        if C % 16:
            return rows.astype(F32).reshape(-1, rows.shape[-1]).astype(BF16)
        return rows.reshape(-1, rows.shape[-1])

    relay, reduce = {}, {}

    def outgoing(b, k, c):
        return pltpu.make_async_remote_copy(
            src_ref=xs[b].at[k, :, chunks[c]], dst_ref=rx[b].at[k, 0, :, chunks[c]],
            send_sem=disp_s.at[b * (E - 1) + k], recv_sem=disp_r.at[b * (E - 1) + k, c],
            device_id=dev(1 - b, k, 0), device_id_type=MESH,
        )

    def share(b, k, c, source):
        for j in range(1, G):
            relay[b, k, j, c] = remote(
                source, rx[b].at[k, j, :, chunks[c]],
                relay_s.at[b, k, j - 1], relay_r.at[b, k, j - 1, c], dev(0, 0, j),
            )

    def pass_on(b, k, c):
        with jax.named_scope(f"pass_{b}_{k}_{c}"):
            outgoing(b, k, c).wait_recv()
            share(b, k, c, rx[b].at[k, 0, :, chunks[c]])

    def arrived(b, k, c):
        with jax.named_scope(f"arr_{b}_{k}_{c}"):
            for j in range(1, G):
                relay[b, k, j, c].wait_recv()

    def put_part(b, k, rows, columns):
        rows = rows.reshape(G, C, rows.shape[-1])
        own[b][k, :, columns] = rows[0]
        for j in range(1, G):
            part[b][k, j, :, columns] = rows[G - j].astype(BF16)

    def send_part(b, k, c):
        for j in range(1, G):
            reduce[b, k, j, c] = remote(
                part[b].at[k, j, :, chunks[c]], rpart[b].at[k, j, :, chunks[c]],
                red_s.at[b, k, j - 1], landed(b, k, j, c), dev(0, 0, j),
            )

    def landed(b, k, j, c):
        return red_r.at[b, k - 1, j - 1, c] if k else near_r.at[b, j - 1]

    def wait_near(b):
        for j in range(1, G):
            whole(
                part[b].at[0, j], rpart[b].at[0, j], red_s.at[b, 0, j - 1], near_r.at[b, j - 1]
            ).wait_recv()

    def summed(b, k, c):
        total = own[b][k, :, chunks[c]]
        for j in range(1, G):
            if k:
                with jax.named_scope(f"red_{b}_{k}_{c}"):
                    reduce[b, k, j, c].wait_recv()
            total = total + rpart[b][k, j, :, chunks[c]].astype(F32)
        return total

    def backward_first(k, c):
        arrived(1, k, c)
        grad = dot_t(flat(rx_b[k, :, :, chunks[c]]), wo[:, chunks[c]])
        sum_b[...] = grad if c == 0 else sum_b[...] + grad

    def backward_hidden(k):
        for j in range(G):
            source = ((e - k + E) % E) * G + (g - j + G) % G
            rows = slice(j * C, (j + 1) * C)
            grad = sum_b[rows, :]
            acts = acts_ref[source].astype(F32)
            gate_act, up_act = acts[:, :F], acts[:, F:]
            squashed = jax.nn.sigmoid(gate_act)
            gate_grad = grad * up_act * squashed * (1.0 + gate_act * (1.0 - squashed))
            both_b[rows, :F] = gate_grad
            both_b[rows, F:] = grad * gate_act * squashed
        joined[...] = both_b[...].astype(BF16)

    def backward_second(k, c):
        for d in range(chunks[c].start, chunks[c].stop, tile_d):
            columns = slice(d, d + tile_d)
            put_part(1, k, dot_t(joined[...], wi[columns, :]), columns)
        send_part(1, k, c)

    def send_back(k, c, h):
        rows = slice(h * half, (h + 1) * half)
        remote(
            pb.at[k, rows, chunks[c]], ret_b.at[k, rows, chunks[c]],
            ret_s.at[k - 1], ret_r.at[k - 1, h], dev(0, -k, 0),
        )

    def backward_return(k, c):
        pb[k, :, chunks[c]] = summed(1, k, c).astype(BF16)
        send_back(k, c, 0)

    def backward_end(k, h):
        low, high = h * half, (h + 1) * half
        if k:
            with jax.named_scope(f"ret_{k}_{h}"):
                rows = slice(low, high)
                whole(
                    pb.at[k, rows], ret_b.at[k, rows], ret_s.at[k - 1], ret_r.at[k - 1, h]
                ).wait_recv()
            pulled = ret_b[k, low:high].astype(F32)
        else:
            pulled = own_b[0, low:high]
            if h == 0:
                with jax.named_scope("red_b0"):
                    wait_near(1)
            for j in range(1, G):
                pulled = pulled + rpart_b[0, j, low:high].astype(F32)
        weighted = gates_b[k * C + low : k * C + high] * pulled * gain_ref[...]
        before = srt[k, low:high].astype(F32)
        inverse = lax.rsqrt(jnp.mean(before * before, axis=-1, keepdims=True) + epsilon)
        unit = before * inverse
        inner = jnp.mean(weighted * unit, axis=-1, keepdims=True)
        th[k, low:high] = (
            xs_b[k, low:high].astype(F32) + inverse * (weighted - unit * inner)
        ).astype(BF16)

    def send_end(k, h):
        rows = slice(h * half, (h + 1) * half)
        remote(th.at[k, rows], fin_b.at[k, rows], out_s.at[k], out_r.at[k], dev(-1, 0, 0))

    detour = pipes > 2 and halves > 1
    low_rows = slice(half, 2 * half)

    cut = tile_d * ((D * 5 // 7) // tile_d)
    by, direct = slice(0, cut), slice(cut, D)

    def by_way(target):
        return whole(via.at[:, by], fin_b.at[0, low_rows, by], via_s, out_r.at[0], target)

    def send_near(h):
        if h != 1 or not detour:
            send_end(0, h)
            return
        pl.when(s != 1)(lambda: send_end(0, h))

        @pl.when(s == 1)
        def _():
            remote(th.at[0, low_rows, by], via.at[:, by], out_s.at[0], via_r, dev(1, 0, 0))
            remote(
                th.at[0, low_rows, direct], fin_b.at[0, low_rows, direct],
                out_s.at[0], out_r.at[0], dev(-1, 0, 0),
            )

    def forward_via():
        if detour:
            @pl.when(s == 2)
            def _():
                whole(th.at[0, low_rows, by], via.at[:, by], out_s.at[0], via_r).wait_recv()
                by_way(dev(-2, 0, 0)).start()

    def forward_first(k, c):
        arrived(0, k, c)
        rows = rx_f[k, :, :, chunks[c]].astype(F32).reshape(G * C, -1)
        lanes = [rows[:, i : i + 128] for i in range(0, rows.shape[1], 128)]
        square = sum(lane * lane for lane in lanes)
        square_f[...] = square if c == 0 else square_f[...] + square
        scaled = (rows * gain_f[:, chunks[c]]).astype(BF16)
        for f in range(0, 2 * F, tile_f):
            hidden = dot(scaled, wi[chunks[c], f : f + tile_f])
            columns = slice(f, f + tile_f)
            sum_f[:, columns] = hidden if c == 0 else sum_f[:, columns] + hidden

    def forward_hidden():
        mean = jnp.sum(square_f[...], axis=-1, keepdims=True) * (1.0 / D)
        inverse = lax.rsqrt(mean + epsilon)
        for f in range(0, F, tile_f):
            gate = sum_f[:, f : f + tile_f] * inverse
            up = sum_f[:, F + f : F + f + tile_f] * inverse
            hidden_ref[:, f : f + tile_f] = (jax.nn.silu(gate) * up).astype(BF16)

    def forward_second(k, c):
        for d in range(chunks[c].start, chunks[c].stop, tile_d):
            columns = slice(d, d + tile_d)
            put_part(0, k, dot(hidden_ref[...], wo[:, columns]), columns)
        send_part(0, k, c)

    def forward_end(k, c):
        total = summed(0, k, c)
        moved = rx_f[k, 0, :, chunks[c]].astype(F32) + rg_f[k][:, :1] * total
        if k == 0:
            fin_f[0, :, chunks[c]] = moved.astype(BF16)
            return
        mv[k, :, chunks[c]] = moved.astype(BF16)
        remote(
            mv.at[k, :, chunks[c]], fin_f.at[k, :, chunks[c]],
            move_s.at[k - 1], move_r.at[k - 1], dev(0, -k, 0),
        )

    tile_f = tile_of(F, 256)
    with jax.named_scope("w_small"):
        for load in (load_gid, *load_small):
            load.wait()
    gather_f, scatter_f = placing(fid_ref[...], e, E, C, us_f.shape[1])
    gather_b, scatter_b = placing(gid_ref[...], e, E, C, us_b.shape[1])
    gather_f_rows, gather_b_rows = gather_f.astype(BF16), gather_b.astype(BF16)
    us_b[...] = scatter_b
    us_f[...] = scatter_f
    gates_b = jnp.sum(gather_b * ggate_ref[...], axis=1, keepdims=True)
    gates_f = jnp.sum(gather_f * fgate_ref[...], axis=1, keepdims=True)
    gs_f[...] = jnp.broadcast_to(gates_f, (T, gs_f.shape[2])).reshape(gs_f.shape)
    early = count // 2
    with jax.named_scope("w_x"):
        load_x.wait()
    for c in range(count):
        xs_f[:, :, chunks[c]] = (
            dot(gather_f_rows, x_ref[:, chunks[c]]).reshape(E, C, -1).astype(BF16)
        )
    with jax.named_scope("w_g"):
        load_g.wait()
    for c in range(count):
        rows = dot(gather_b_rows, g_ref[:, chunks[c]]).reshape(E, C, -1).astype(BF16)
        xs_b[:, :, chunks[c]] = rows
        rx_b[0, 0, :, chunks[c]] = rows[0]
    with jax.named_scope("w_bar"):
        pl.semaphore_wait(barrier, len(near) + E * (1 + (s + pipes - 1) // pipes))
    gain_copy = remote(gain_ref, gain_f, perm_s.at[2], perm_r.at[2], dev(1, 0, 0))
    for k in range(E):
        remote(gs_f.at[k], rg_f.at[k], gate_s, gate_r, dev(1, k, 0))
    perm_f = remote(us_f, ur_f, perm_s.at[0], perm_r.at[0], dev(1, 0, 0))

    def send_forward(order):
        for k, c in order:
            outgoing(0, k, c).start()

    far = [(k, c) for k in others for c in range(count)]
    own_rows = [(0, c) for c in range(count)]
    pl.when(s != pipes - 1)(lambda: send_forward(own_rows + far))
    pl.when(last)(lambda: send_forward(own_rows[-1:] + far + own_rows[:-1]))
    for c in range(count):
        for k in others:
            outgoing(1, k, c).start()
    for c in range(count):
        share(1, 0, c, xs_b.at[0, :, chunks[c]])
    pl.when(last)(lambda: greet(ready_sem, following))
    with jax.named_scope("w_saved"):
        load_saved.wait()
    srt[...] = dot(gather_b_rows, saved_ref[...]).reshape(E, C, D).astype(BF16)

    with jax.named_scope("w_wo"):
        load_wo.wait()
        load_acts.wait()
    with jax.named_scope("b1_0"):
        for c in range(count):
            backward_first(0, c)
        backward_hidden(0)
    with jax.named_scope("w_wi"):
        load_wi.wait()

    def near_end():
        whole(us_b, ur_b, perm_s.at[1], perm_r.at[1], dev(-1, 0, 0)).start()
        for h in range(halves):
            send_near(h)

    def last_ends():
        for k in others:
            for h in range(1, halves):
                with jax.named_scope(f"bend1_{h}"):
                    backward_end(k, h)
                    send_end(k, h)

    for c in range(count):
        with jax.named_scope(f"b2_0_{c}"):
            backward_second(0, c)
        if 1 <= c <= early:
            for k in others:
                pass_on(1, k, c - 1)
    for c in range(early):
        with jax.named_scope(f"b1_1a{c}"):
            backward_first(1, c)
        if c == 0:
            for k in others:
                for i in range(early, count - 1):
                    pass_on(1, k, i)
    for k in others:
        pass_on(1, k, count - 1)
    with jax.named_scope("bend0"):
        for h in range(halves):
            backward_end(0, h)
    for k in others:
        with jax.named_scope("b1_1b"):
            for c in range(early if k == 1 else 0, count):
                backward_first(k, c)
            backward_hidden(k)
        for c in range(count):
            with jax.named_scope(f"b2_1_{c}"):
                backward_second(k, c)
            if k == 1 and c == max(early - 1, 0):
                pl.when(s != 0)(near_end)
            if k == E - 1 and c >= early > 0:
                for other in others:
                    pass_on(0, other, c - early)
            if c >= 1:
                with jax.named_scope(f"bret_{c - 1}"):
                    backward_return(k, c - 1)
        if k == E - 1:
            for other in others:
                for c in range(early, count - 1):
                    pass_on(0, other, c)
        with jax.named_scope(f"bret_{count - 1}"):
            backward_return(k, count - 1)
        if k == E - 1:
            for other in others:
                pass_on(0, other, count - 1)
        for h in range(1, halves):
            for c in range(count):
                send_back(k, c, h)
    with jax.named_scope("w_gain"):
        gain_copy.wait_recv()
    with jax.named_scope("w_prev"):
        pl.when(first)(lambda: pl.semaphore_wait(ready_sem, E))
        pl.when(first)(near_end)
    with jax.named_scope("w_gate"):
        whole(gs_f, rg_f, gate_s, gate_r).wait_recv()
    for k in others:
        for c in range(count):
            with jax.named_scope(f"f1_1_{c}"):
                forward_first(k, c)
        with jax.named_scope("fh_1"):
            forward_hidden()
        if k == 1:
            with jax.named_scope("w_via"):
                forward_via()
        for c in range(count):
            with jax.named_scope(f"f2_1_{c}"):
                forward_second(k, c)
            if c == max(LAG, count - 2) or count == 1:
                with jax.named_scope("bend1_0"):
                    backward_end(k, 0)
                    send_end(k, 0)
            if c >= LAG:
                with jax.named_scope(f"fend_1_{c - LAG}"):
                    forward_end(k, c - LAG)
        if k == E - 1:
            for c in range(count):
                pass_on(0, 0, c)
        for c in range(max(count - LAG, 0), count):
            with jax.named_scope(f"fend_1_{c}"):
                forward_end(k, c)
    for c in range(count):
        with jax.named_scope(f"f1_0_{c}"):
            forward_first(0, c)
        if c == early - 1:
            last_ends()
    with jax.named_scope("fh_0"):
        forward_hidden()
    with jax.named_scope("f2_0"):
        for c in range(count):
            forward_second(0, c)
    if early == 0:
        last_ends()
    with jax.named_scope("fend0"):
        wait_near(0)
        for c in range(count):
            forward_end(0, c)

    with jax.named_scope("w_perm"):
        perm_f.wait_recv()
        whole(us_b, ur_b, perm_s.at[1], perm_r.at[1]).wait_recv()
    for k in others:
        with jax.named_scope("w_move"):
            whole(mv.at[k], fin_f.at[k], move_s.at[k - 1], move_r.at[k - 1]).wait_recv()
    for k in range(E):
        with jax.named_scope(f"w_out{k}"):
            whole(th.at[k], fin_b.at[k], out_s.at[k], out_r.at[k]).wait_recv()
    with jax.named_scope("w_sends"):
        for b in range(2):
            for k in range(b, E):
                i = b * (E - 1) + k
                whole(xs[b].at[k], rx[b].at[k, 0], disp_s.at[i], disp_r.at[i, 0]).wait_send()
            for k in range(E):
                for j in range(1, G):
                    i = (b, k, j - 1)
                    whole(
                        rx[b].at[k, 0], rx[b].at[k, j], relay_s.at[i], relay_r.at[(*i, 0)]
                    ).wait_send()
                    whole(part[b].at[k, j], rpart[b].at[k, j], red_s.at[i], near_r.at[b, j - 1]).wait_send()
        for k in others:
            whole(pb.at[k], ret_b.at[k], ret_s.at[k - 1], ret_r.at[k - 1, 0]).wait_send()
            whole(mv.at[k], fin_f.at[k], move_s.at[k - 1], move_r.at[k - 1]).wait_send()
        for k in range(E):
            whole(th.at[k], fin_b.at[k], out_s.at[k], out_r.at[k]).wait_send()
        whole(gs_f, rg_f, gate_s, gate_r).wait_send()
        if detour:
            pl.when(s == 2)(lambda: by_way(dev(-2, 0, 0)).wait_send())
        for copy in (gain_copy, perm_f, whole(us_b, ur_b, perm_s.at[1], perm_r.at[1])):
            copy.wait_send()


UNSORT_STEPS = 2


def unsort(fin_f, fin_b, ur_f, ur_b, fout_hbm, gout_hbm, held, sems):
    T, D = fout_hbm.shape
    width = D // UNSORT_STEPS
    copies = []
    for i, (fin, ur, out) in enumerate(((fin_f, ur_f, fout_hbm), (fin_b, ur_b, gout_hbm))):
        for c in range(UNSORT_STEPS):
            columns = pl.ds(c * width, width)
            rows = fin[:, :, columns].astype(F32).reshape(T, width).astype(BF16)
            held[i, :, columns] = dot(ur[:, :T], rows).astype(BF16)
            copy = pltpu.make_async_copy(held.at[i, :, columns], out.at[:, columns], sems.at[i, c])
            copy.start()
            copies.append(copy)
    for copy in copies:
        copy.wait()


def on_device(
    dims,
    forward_in,
    forward_ids,
    forward_gates,
    grad_in,
    grad_ids,
    grad_gates,
    saved_input,
    saved_acts,
    norm_gain,
    weight_in,
    weight_out,
):
    pipes, E, G = dims
    T, D = forward_in.shape[1:]
    F = weight_out.shape[1]
    C = T // E
    padded = -(-T // 128) * 128
    DMA = pltpu.SemaphoreType.DMA
    rows = (E, C, D)
    vmem = pl.BlockSpec(memory_space=pltpu.VMEM)
    hbm = pl.BlockSpec(memory_space=pl.ANY)
    sorted_rows = jax.ShapeDtypeStruct(rows, BF16)
    order = jax.ShapeDtypeStruct((T, padded), BF16)
    halves, N = disp_rows(C), len(columns_of(D, C))
    arrived = pl.pallas_call(
        functools.partial(kernel, dims),
        out_shape=(pltpu.VMEM(rows, BF16), pltpu.VMEM(rows, BF16), pltpu.VMEM((T, padded), BF16), pltpu.VMEM((T, padded), BF16)),
        in_specs=[hbm] * 11,
        out_specs=(vmem, vmem, vmem, vmem),
        scratch_shapes=[
            pltpu.VMEM((1, T), jnp.int32), pltpu.VMEM((1, T), F32),
            pltpu.VMEM((1, T), jnp.int32), pltpu.VMEM((1, T), F32),
            pltpu.VMEM((1, D), F32),
            pltpu.VMEM((T, D), BF16), pltpu.VMEM((T, D), BF16), pltpu.VMEM((T, D), BF16),
            pltpu.VMEM((E * G, C, 2 * F), BF16),
            pltpu.VMEM((D, 2 * F), BF16),
            pltpu.VMEM((F, D), BF16),
            pltpu.VMEM((1, D), F32),
            pltpu.VMEM(rows, BF16), pltpu.VMEM(rows, BF16),
            pltpu.VMEM((E, G, C, D), BF16), pltpu.VMEM((E, G, C, D), BF16),
            pltpu.VMEM((E, C, 128), F32), pltpu.VMEM((E, C, 128), F32),
            pltpu.VMEM((T, padded), BF16), pltpu.VMEM((T, padded), BF16),
            pltpu.VMEM((E, G, C, D), BF16), pltpu.VMEM((E, G, C, D), BF16),
            pltpu.VMEM((E, G, C, D), BF16), pltpu.VMEM((E, G, C, D), BF16),
            pltpu.VMEM(rows, F32), pltpu.VMEM(rows, F32),
            pltpu.VMEM(rows, BF16), pltpu.VMEM(rows, BF16), pltpu.VMEM(rows, BF16),
            pltpu.VMEM(rows, BF16), pltpu.VMEM(rows, BF16),
            pltpu.VMEM((G * C, F), BF16),
            pltpu.VMEM((G * C, 2 * F), BF16),
            pltpu.VMEM((G * C, F), F32), pltpu.VMEM((G * C, 2 * F), F32),
            pltpu.VMEM((G * C, 2 * F), F32), pltpu.VMEM((G * C, 128), F32),
            pltpu.VMEM((C // halves, D), BF16),
            DMA((11,)), pltpu.SemaphoreType.REGULAR, DMA, DMA,
            DMA((2 * E - 1,)), DMA((2 * E - 1, N)), DMA, DMA,
            DMA((2, E, G - 1)), DMA((2, E, G - 1, N)), DMA((3,)), DMA((3,)),
            DMA((2, E, G - 1)), DMA((2, E - 1, G - 1, N)), DMA((2, G - 1)),
            DMA((E - 1,)), DMA((E - 1,)), DMA((E,)), DMA((E,)),
            DMA((E - 1,)), DMA((E - 1, halves)),
        ],
        compiler_params=pltpu.CompilerParams(
            collective_id=0, has_side_effects=True, vmem_limit_bytes=40 * 2**20
        ),
    )(*[
        pltpu.with_memory_space_constraint(a, pltpu.HBM)
        for a in (
            forward_ids.reshape(1, T),
            forward_gates.reshape(1, T),
            grad_ids.reshape(1, T),
            grad_gates.reshape(1, T),
            norm_gain,
            forward_in[0],
            grad_in[0],
            saved_input[0],
            saved_acts.reshape(E * G, C, 2 * F),
            weight_in[0],
            weight_out[0],
        )
    ])
    out_shape = jax.ShapeDtypeStruct((T, D), BF16)
    fwd, grad = pl.pallas_call(
        unsort,
        out_shape=(out_shape, out_shape),
        in_specs=[vmem] * 4,
        out_specs=(hbm, hbm),
        scratch_shapes=[pltpu.VMEM((2, T, D), BF16), DMA((2, UNSORT_STEPS))],
        compiler_params=pltpu.CompilerParams(vmem_limit_bytes=8 * 2**20),
    )(*[pltpu.with_memory_space_constraint(a, pltpu.VMEM) for a in arrived])
    return fwd[None], grad[None]


def solution(mesh):
    sources = mesh.shape["expert"]
    G = min(4, sources // 2)
    dims = (mesh.shape["pipe"], sources // G, G)
    placed = (
        P("pipe", "expert", None),
        P("pipe", "expert", None),
        P("pipe", "expert", None),
        P("pipe", "expert", None),
        P("pipe", "expert", None),
        P("pipe", "expert", None),
        P("pipe", "expert", None),
        P("pipe", "expert", None, None),
        P("pipe", None),
        P("expert", None, None),
        P("expert", None, None),
    )
    return jax.shard_map(
        functools.partial(on_device, dims),
        mesh=mesh,
        in_specs=placed,
        out_specs=(P("pipe", "expert", None), P("pipe", "expert", None)),
        check_vma=False,
    )
```

```python
import contextlib
import functools

import jax
import jax.numpy as jnp
from jax import lax
from jax.experimental import pallas as pl
from jax.experimental.pallas import tpu as pltpu
from jax.sharding import PartitionSpec as P

epsilon = 1e-06
F32 = jnp.float32
BF16 = jnp.bfloat16
MESH = pl.DeviceIdType.MESH


@contextlib.contextmanager
def stage(name):
    with jax.named_scope(name):
        pl.delay(1)
        yield


def tile_of(width, most):
    tile = most
    while width % tile:
        tile //= 2
    return tile


LAG = 2


def disp_rows(C):
    return 2 if C % 32 == 0 else 1


def columns_of(D, C):
    tile = tile_of(D, 512)
    tiles = D // tile
    width = tile * (-(-tiles // 4) if C % 32 == 0 else tiles)
    return [slice(d, min(d + width, D)) for d in range(0, D, width)]


def dot(a, b):
    return lax.dot_general(a, b, (((1,), (0,)), ((), ())), preferred_element_type=F32)


def dot_t(a, b):
    return lax.dot_general(a, b, (((1,), (1,)), ((), ())), preferred_element_type=F32)


def placing(ids_row, own, experts, capacity, padded):
    count = ids_row.shape[1]
    down = lax.broadcasted_iota(jnp.int32, (count, count), 0)
    across = lax.broadcasted_iota(jnp.int32, (count, count), 1)
    rel = ids_row - own
    rel = jnp.where(rel < 0, rel + experts, rel).astype(F32)
    spread = jnp.broadcast_to(rel, (count, count))
    column = jnp.sum(jnp.where(down == across, spread, 0.0), axis=1, keepdims=True)
    before = jnp.where((column == spread) & (down < across), 1.0, 0.0)
    rank = jnp.sum(before, axis=0, keepdims=True)
    slot = jnp.broadcast_to(rel * capacity + rank, (count, count))
    slot_column = jnp.sum(jnp.where(down == across, slot, 0.0), axis=1, keepdims=True)
    gather = jnp.where(down.astype(F32) == slot, 1.0, 0.0)
    wide = lax.broadcasted_iota(jnp.int32, (count, padded), 1).astype(F32)
    scatter = jnp.where(slot_column == wide, 1.0, 0.0).astype(BF16)
    return gather, scatter


def kernel(
    dims,
    fid_hbm, fgate_hbm, gid_hbm, ggate_hbm, gain_hbm,
    x_hbm, g_hbm, saved_hbm, acts_hbm, wi_hbm, wo_hbm,
    fin_f, fin_b, ur_f, ur_b,
    fid_ref, fgate_ref, gid_ref, ggate_ref, gain_ref,
    x_ref, g_ref, saved_ref, acts_ref, wi, wo, gain_f,
    xs_f, xs_b, rx_f, rx_b, gs_f, rg_f, us_f, us_b,
    part_f, part_b, rpart_f, rpart_b, own_f, own_b,
    mv, pb, ret_b, th, srt, hidden_ref, joined, sum_b, both_b, sum_f, square_f,
    via, w_sem, ready_sem, via_s, via_r,
    disp_s, disp_r, gate_s, gate_r, relay_s, relay_r, perm_s, perm_r, red_s, red_r, near_r,
    move_s, move_r, out_s, out_r, ret_s, ret_r,
):
    pipes, E, G = dims
    s = lax.axis_index("pipe")
    position = lax.axis_index("expert")
    e = position // G
    g = position % G
    C, D = xs_f.shape[1:]
    T = x_ref.shape[0]
    F = wo.shape[0]

    def dev(hop, k, j):
        return (
            (s + hop + pipes) % pipes,
            ((e + k + E) % E) * G + (g + j + G) % G,
        )

    near = [dev(0, k, 0) for k in range(1, E)] + [dev(0, 0, j) for j in range(1, G)]
    following = [dev(1, k, 0) for k in range(E)]
    previous = [dev(-1, k, 0) for k in range(E)]
    first, last = s == 0, s == pipes - 1

    def greet(sem, peers):
        for peer in peers:
            pl.semaphore_signal(sem, inc=1, device_id=peer, device_id_type=MESH)

    barrier = pltpu.get_barrier_semaphore()
    greet(barrier, near)
    greet(barrier, previous)
    pl.when(s != pipes - 1)(lambda: greet(barrier, following))
    pairs = (
        (gid_hbm, gid_ref), (g_hbm, g_ref), (fid_hbm, fid_ref), (fgate_hbm, fgate_ref),
        (ggate_hbm, ggate_ref), (gain_hbm, gain_ref), (x_hbm, x_ref), (saved_hbm, saved_ref), (acts_hbm, acts_ref),
        (wo_hbm, wo), (wi_hbm, wi),
    )
    loads = [
        pltpu.make_async_copy(source, held, w_sem.at[i]) for i, (source, held) in enumerate(pairs)
    ]
    for load in loads:
        load.start()
    load_gid, load_g, *load_small, load_x, load_saved, load_acts, load_wo, load_wi = loads

    def remote(src, dst, send, recv, target):
        copy = pltpu.make_async_remote_copy(
            src_ref=src, dst_ref=dst, send_sem=send, recv_sem=recv,
            device_id=target, device_id_type=MESH,
        )
        copy.start()
        return copy

    def whole(src, dst, send, recv, target=None):
        return pltpu.make_async_remote_copy(
            src_ref=src, dst_ref=dst, send_sem=send, recv_sem=recv,
            device_id=dev(1, 0, 0) if target is None else target, device_id_type=MESH,
        )

    xs, rx = (xs_f, xs_b), (rx_f, rx_b)
    part, rpart = (part_f, part_b), (rpart_f, rpart_b)
    own = (own_f, own_b)
    halves = disp_rows(C)
    half = C // halves
    tile_d = tile_of(D, 512)
    chunks = columns_of(D, C)
    count = len(chunks)
    others = range(1, E)

    def flat(rows):
        if C % 16:
            return rows.astype(F32).reshape(-1, rows.shape[-1]).astype(BF16)
        return rows.reshape(-1, rows.shape[-1])

    relay, reduce = {}, {}

    def outgoing(b, k, c):
        return pltpu.make_async_remote_copy(
            src_ref=xs[b].at[k, :, chunks[c]], dst_ref=rx[b].at[k, 0, :, chunks[c]],
            send_sem=disp_s.at[b * (E - 1) + k], recv_sem=disp_r.at[b * (E - 1) + k, c],
            device_id=dev(1 - b, k, 0), device_id_type=MESH,
        )

    def share(b, k, c, source):
        for j in range(1, G):
            relay[b, k, j, c] = remote(
                source, rx[b].at[k, j, :, chunks[c]],
                relay_s.at[b, k, j - 1], relay_r.at[b, k, j - 1, c], dev(0, 0, j),
            )

    def pass_on(b, k, c):
        with jax.named_scope(f"pass_{b}_{k}_{c}"):
            outgoing(b, k, c).wait_recv()
            share(b, k, c, rx[b].at[k, 0, :, chunks[c]])

    def arrived(b, k, c):
        with jax.named_scope(f"arr_{b}_{k}_{c}"):
            for j in range(1, G):
                relay[b, k, j, c].wait_recv()

    def put_part(b, k, rows, columns):
        rows = rows.reshape(G, C, rows.shape[-1])
        own[b][k, :, columns] = rows[0]
        for j in range(1, G):
            part[b][k, j, :, columns] = rows[G - j].astype(BF16)

    def send_part(b, k, c):
        for j in range(1, G):
            reduce[b, k, j, c] = remote(
                part[b].at[k, j, :, chunks[c]], rpart[b].at[k, j, :, chunks[c]],
                red_s.at[b, k, j - 1], landed(b, k, j, c), dev(0, 0, j),
            )

    def landed(b, k, j, c):
        return red_r.at[b, k - 1, j - 1, c] if k else near_r.at[b, j - 1]

    def wait_near(b):
        for j in range(1, G):
            whole(
                part[b].at[0, j], rpart[b].at[0, j], red_s.at[b, 0, j - 1], near_r.at[b, j - 1]
            ).wait_recv()

    def summed(b, k, c):
        total = own[b][k, :, chunks[c]]
        for j in range(1, G):
            if k:
                with jax.named_scope(f"red_{b}_{k}_{c}"):
                    reduce[b, k, j, c].wait_recv()
            total = total + rpart[b][k, j, :, chunks[c]].astype(F32)
        return total

    def backward_first(k, c):
        arrived(1, k, c)
        grad = dot_t(flat(rx_b[k, :, :, chunks[c]]), wo[:, chunks[c]])
        sum_b[...] = grad if c == 0 else sum_b[...] + grad

    def backward_hidden(k):
        for j in range(G):
            source = ((e - k + E) % E) * G + (g - j + G) % G
            rows = slice(j * C, (j + 1) * C)
            grad = sum_b[rows, :]
            acts = acts_ref[source].astype(F32)
            gate_act, up_act = acts[:, :F], acts[:, F:]
            squashed = jax.nn.sigmoid(gate_act)
            gate_grad = grad * up_act * squashed * (1.0 + gate_act * (1.0 - squashed))
            both_b[rows, :F] = gate_grad
            both_b[rows, F:] = grad * gate_act * squashed
        joined[...] = both_b[...].astype(BF16)

    def backward_second(k, c):
        for d in range(chunks[c].start, chunks[c].stop, tile_d):
            columns = slice(d, d + tile_d)
            put_part(1, k, dot_t(joined[...], wi[columns, :]), columns)
        send_part(1, k, c)

    def send_back(k, c, h):
        rows = slice(h * half, (h + 1) * half)
        remote(
            pb.at[k, rows, chunks[c]], ret_b.at[k, rows, chunks[c]],
            ret_s.at[k - 1], ret_r.at[k - 1, h], dev(0, -k, 0),
        )

    def backward_return(k, c):
        pb[k, :, chunks[c]] = summed(1, k, c).astype(BF16)
        send_back(k, c, 0)

    def backward_end(k, h):
        low, high = h * half, (h + 1) * half
        if k:
            with stage(f"ret_{k}_{h}"):
                rows = slice(low, high)
                whole(
                    pb.at[k, rows], ret_b.at[k, rows], ret_s.at[k - 1], ret_r.at[k - 1, h]
                ).wait_recv()
            pulled = ret_b[k, low:high].astype(F32)
        else:
            pulled = own_b[0, low:high]
            if h == 0:
                with jax.named_scope("red_b0"):
                    wait_near(1)
            for j in range(1, G):
                pulled = pulled + rpart_b[0, j, low:high].astype(F32)
        weighted = gates_b[k * C + low : k * C + high] * pulled * gain_ref[...]
        before = srt[k, low:high].astype(F32)
        inverse = lax.rsqrt(jnp.mean(before * before, axis=-1, keepdims=True) + epsilon)
        unit = before * inverse
        inner = jnp.mean(weighted * unit, axis=-1, keepdims=True)
        th[k, low:high] = (
            xs_b[k, low:high].astype(F32) + inverse * (weighted - unit * inner)
        ).astype(BF16)

    def send_end(k, h):
        rows = slice(h * half, (h + 1) * half)
        remote(th.at[k, rows], fin_b.at[k, rows], out_s.at[k], out_r.at[k], dev(-1, 0, 0))

    detour = pipes > 2 and halves > 1
    low_rows = slice(half, 2 * half)

    cut = tile_d * ((D * 5 // 7) // tile_d)
    by, direct = slice(0, cut), slice(cut, D)

    def by_way(target):
        return whole(via.at[:, by], fin_b.at[0, low_rows, by], via_s, out_r.at[0], target)

    def send_near(h):
        if h != 1 or not detour:
            send_end(0, h)
            return
        pl.when(s != 1)(lambda: send_end(0, h))

        @pl.when(s == 1)
        def _():
            remote(th.at[0, low_rows, by], via.at[:, by], out_s.at[0], via_r, dev(1, 0, 0))
            remote(
                th.at[0, low_rows, direct], fin_b.at[0, low_rows, direct],
                out_s.at[0], out_r.at[0], dev(-1, 0, 0),
            )

    def forward_via():
        if detour:
            @pl.when(s == 2)
            def _():
                whole(th.at[0, low_rows, by], via.at[:, by], out_s.at[0], via_r).wait_recv()
                by_way(dev(-2, 0, 0)).start()

    def forward_first(k, c):
        arrived(0, k, c)
        rows = rx_f[k, :, :, chunks[c]].astype(F32).reshape(G * C, -1)
        lanes = [rows[:, i : i + 128] for i in range(0, rows.shape[1], 128)]
        square = sum(lane * lane for lane in lanes)
        square_f[...] = square if c == 0 else square_f[...] + square
        scaled = (rows * gain_f[:, chunks[c]]).astype(BF16)
        for f in range(0, 2 * F, tile_f):
            hidden = dot(scaled, wi[chunks[c], f : f + tile_f])
            columns = slice(f, f + tile_f)
            sum_f[:, columns] = hidden if c == 0 else sum_f[:, columns] + hidden

    def forward_hidden():
        mean = jnp.sum(square_f[...], axis=-1, keepdims=True) * (1.0 / D)
        inverse = lax.rsqrt(mean + epsilon)
        for f in range(0, F, tile_f):
            gate = sum_f[:, f : f + tile_f] * inverse
            up = sum_f[:, F + f : F + f + tile_f] * inverse
            hidden_ref[:, f : f + tile_f] = (jax.nn.silu(gate) * up).astype(BF16)

    def forward_second(k, c):
        for d in range(chunks[c].start, chunks[c].stop, tile_d):
            columns = slice(d, d + tile_d)
            put_part(0, k, dot(hidden_ref[...], wo[:, columns]), columns)
        send_part(0, k, c)

    def forward_end(k, c):
        total = summed(0, k, c)
        moved = rx_f[k, 0, :, chunks[c]].astype(F32) + rg_f[k][:, :1] * total
        if k == 0:
            fin_f[0, :, chunks[c]] = moved.astype(BF16)
            return
        mv[k, :, chunks[c]] = moved.astype(BF16)
        remote(
            mv.at[k, :, chunks[c]], fin_f.at[k, :, chunks[c]],
            move_s.at[k - 1], move_r.at[k - 1], dev(0, -k, 0),
        )

    tile_f = tile_of(F, 256)
    with jax.named_scope("w_small"):
        for load in (load_gid, *load_small):
            load.wait()
    gather_f, scatter_f = placing(fid_ref[...], e, E, C, us_f.shape[1])
    gather_b, scatter_b = placing(gid_ref[...], e, E, C, us_b.shape[1])
    gather_f_rows, gather_b_rows = gather_f.astype(BF16), gather_b.astype(BF16)
    us_b[...] = scatter_b
    us_f[...] = scatter_f
    gates_b = jnp.sum(gather_b * ggate_ref[...], axis=1, keepdims=True)
    gates_f = jnp.sum(gather_f * fgate_ref[...], axis=1, keepdims=True)
    gs_f[...] = jnp.broadcast_to(gates_f, (T, gs_f.shape[2])).reshape(gs_f.shape)
    early = count // 2
    with jax.named_scope("w_x"):
        load_x.wait()
    for c in range(count):
        xs_f[:, :, chunks[c]] = (
            dot(gather_f_rows, x_ref[:, chunks[c]]).reshape(E, C, -1).astype(BF16)
        )
    with jax.named_scope("w_g"):
        load_g.wait()
    for c in range(count):
        rows = dot(gather_b_rows, g_ref[:, chunks[c]]).reshape(E, C, -1).astype(BF16)
        xs_b[:, :, chunks[c]] = rows
        rx_b[0, 0, :, chunks[c]] = rows[0]
    with jax.named_scope("w_bar"):
        pl.semaphore_wait(barrier, len(near) + E * (1 + (s + pipes - 1) // pipes))
    gain_copy = remote(gain_ref, gain_f, perm_s.at[2], perm_r.at[2], dev(1, 0, 0))
    for k in range(E):
        remote(gs_f.at[k], rg_f.at[k], gate_s, gate_r, dev(1, k, 0))
    perm_f = remote(us_f, ur_f, perm_s.at[0], perm_r.at[0], dev(1, 0, 0))

    def send_forward(order):
        for k, c in order:
            outgoing(0, k, c).start()

    far = [(k, c) for k in others for c in range(count)]
    own_rows = [(0, c) for c in range(count)]
    pl.when(s != pipes - 1)(lambda: send_forward(own_rows + far))
    pl.when(last)(lambda: send_forward(own_rows[-1:] + far + own_rows[:-1]))
    for c in range(count):
        for k in others:
            outgoing(1, k, c).start()
    for c in range(count):
        share(1, 0, c, xs_b.at[0, :, chunks[c]])
    pl.when(last)(lambda: greet(ready_sem, following))
    with jax.named_scope("w_saved"):
        load_saved.wait()
    srt[...] = dot(gather_b_rows, saved_ref[...]).reshape(E, C, D).astype(BF16)

    with jax.named_scope("w_wo"):
        load_wo.wait()
        load_acts.wait()
    with stage("b1_0"):
        for c in range(count):
            backward_first(0, c)
        backward_hidden(0)
    with jax.named_scope("w_wi"):
        load_wi.wait()

    def near_end():
        whole(us_b, ur_b, perm_s.at[1], perm_r.at[1], dev(-1, 0, 0)).start()
        for h in range(halves):
            send_near(h)

    def last_ends():
        for k in others:
            for h in range(1, halves):
                with stage(f"bend1_{h}"):
                    backward_end(k, h)
                    send_end(k, h)

    for c in range(count):
        with stage(f"b2_0_{c}"):
            backward_second(0, c)
        if 1 <= c <= early:
            for k in others:
                pass_on(1, k, c - 1)
    for c in range(early):
        with stage(f"b1_1a{c}"):
            backward_first(1, c)
        if c == 0:
            for k in others:
                for i in range(early, count - 1):
                    pass_on(1, k, i)
    for k in others:
        pass_on(1, k, count - 1)
    with stage("bend0"):
        for h in range(halves):
            backward_end(0, h)
    for k in others:
        with stage("b1_1b"):
            for c in range(early if k == 1 else 0, count):
                backward_first(k, c)
            backward_hidden(k)
        for c in range(count):
            with stage(f"b2_1_{c}"):
                backward_second(k, c)
            if k == 1 and c == max(early - 1, 0):
                pl.when(s != 0)(near_end)
            if k == E - 1 and c >= early > 0:
                for other in others:
                    pass_on(0, other, c - early)
            if c >= 1:
                with stage(f"bret_{c - 1}"):
                    backward_return(k, c - 1)
        if k == E - 1:
            for other in others:
                for c in range(early, count - 1):
                    pass_on(0, other, c)
        with stage(f"bret_{count - 1}"):
            backward_return(k, count - 1)
        if k == E - 1:
            for other in others:
                pass_on(0, other, count - 1)
        for h in range(1, halves):
            for c in range(count):
                send_back(k, c, h)
    with jax.named_scope("w_gain"):
        gain_copy.wait_recv()
    with jax.named_scope("w_prev"):
        pl.when(first)(lambda: pl.semaphore_wait(ready_sem, E))
        pl.when(first)(near_end)
    with jax.named_scope("w_gate"):
        whole(gs_f, rg_f, gate_s, gate_r).wait_recv()
    for k in others:
        for c in range(count):
            with stage(f"f1_1_{c}"):
                forward_first(k, c)
        with stage("fh_1"):
            forward_hidden()
        if k == 1:
            with jax.named_scope("w_via"):
                forward_via()
        for c in range(count):
            with stage(f"f2_1_{c}"):
                forward_second(k, c)
            if c == max(LAG, count - 2) or count == 1:
                with stage("bend1_0"):
                    backward_end(k, 0)
                    send_end(k, 0)
            if c >= LAG:
                with stage(f"fend_1_{c - LAG}"):
                    forward_end(k, c - LAG)
        if k == E - 1:
            for c in range(count):
                pass_on(0, 0, c)
        for c in range(max(count - LAG, 0), count):
            with stage(f"fend_1_{c}"):
                forward_end(k, c)
    for c in range(count):
        with stage(f"f1_0_{c}"):
            forward_first(0, c)
        if c == early - 1:
            last_ends()
    with stage("fh_0"):
        forward_hidden()
    with stage("f2_0"):
        for c in range(count):
            forward_second(0, c)
    if early == 0:
        last_ends()
    with stage("fend0"):
        wait_near(0)
        for c in range(count):
            forward_end(0, c)

    with jax.named_scope("w_perm"):
        perm_f.wait_recv()
        whole(us_b, ur_b, perm_s.at[1], perm_r.at[1]).wait_recv()
    for k in others:
        with jax.named_scope("w_move"):
            whole(mv.at[k], fin_f.at[k], move_s.at[k - 1], move_r.at[k - 1]).wait_recv()
    for k in range(E):
        with jax.named_scope(f"w_out{k}"):
            whole(th.at[k], fin_b.at[k], out_s.at[k], out_r.at[k]).wait_recv()
    with jax.named_scope("w_sends"):
        for b in range(2):
            for k in range(b, E):
                i = b * (E - 1) + k
                whole(xs[b].at[k], rx[b].at[k, 0], disp_s.at[i], disp_r.at[i, 0]).wait_send()
            for k in range(E):
                for j in range(1, G):
                    i = (b, k, j - 1)
                    whole(
                        rx[b].at[k, 0], rx[b].at[k, j], relay_s.at[i], relay_r.at[(*i, 0)]
                    ).wait_send()
                    whole(part[b].at[k, j], rpart[b].at[k, j], red_s.at[i], near_r.at[b, j - 1]).wait_send()
        for k in others:
            whole(pb.at[k], ret_b.at[k], ret_s.at[k - 1], ret_r.at[k - 1, 0]).wait_send()
            whole(mv.at[k], fin_f.at[k], move_s.at[k - 1], move_r.at[k - 1]).wait_send()
        for k in range(E):
            whole(th.at[k], fin_b.at[k], out_s.at[k], out_r.at[k]).wait_send()
        whole(gs_f, rg_f, gate_s, gate_r).wait_send()
        if detour:
            pl.when(s == 2)(lambda: by_way(dev(-2, 0, 0)).wait_send())
        for copy in (gain_copy, perm_f, whole(us_b, ur_b, perm_s.at[1], perm_r.at[1])):
            copy.wait_send()


UNSORT_STEPS = 2


def unsort(fin_f, fin_b, ur_f, ur_b, fout_hbm, gout_hbm, held, sems):
    T, D = fout_hbm.shape
    width = D // UNSORT_STEPS
    copies = []
    for i, (fin, ur, out) in enumerate(((fin_f, ur_f, fout_hbm), (fin_b, ur_b, gout_hbm))):
        for c in range(UNSORT_STEPS):
            columns = pl.ds(c * width, width)
            rows = fin[:, :, columns].astype(F32).reshape(T, width).astype(BF16)
            held[i, :, columns] = dot(ur[:, :T], rows).astype(BF16)
            copy = pltpu.make_async_copy(held.at[i, :, columns], out.at[:, columns], sems.at[i, c])
            copy.start()
            copies.append(copy)
    for copy in copies:
        copy.wait()


def on_device(
    dims,
    forward_in,
    forward_ids,
    forward_gates,
    grad_in,
    grad_ids,
    grad_gates,
    saved_input,
    saved_acts,
    norm_gain,
    weight_in,
    weight_out,
):
    pipes, E, G = dims
    T, D = forward_in.shape[1:]
    F = weight_out.shape[1]
    C = T // E
    padded = -(-T // 128) * 128
    DMA = pltpu.SemaphoreType.DMA
    rows = (E, C, D)
    vmem = pl.BlockSpec(memory_space=pltpu.VMEM)
    hbm = pl.BlockSpec(memory_space=pl.ANY)
    sorted_rows = jax.ShapeDtypeStruct(rows, BF16)
    order = jax.ShapeDtypeStruct((T, padded), BF16)
    halves, N = disp_rows(C), len(columns_of(D, C))
    arrived = pl.pallas_call(
        functools.partial(kernel, dims),
        out_shape=(pltpu.VMEM(rows, BF16), pltpu.VMEM(rows, BF16), pltpu.VMEM((T, padded), BF16), pltpu.VMEM((T, padded), BF16)),
        in_specs=[hbm] * 11,
        out_specs=(vmem, vmem, vmem, vmem),
        scratch_shapes=[
            pltpu.VMEM((1, T), jnp.int32), pltpu.VMEM((1, T), F32),
            pltpu.VMEM((1, T), jnp.int32), pltpu.VMEM((1, T), F32),
            pltpu.VMEM((1, D), F32),
            pltpu.VMEM((T, D), BF16), pltpu.VMEM((T, D), BF16), pltpu.VMEM((T, D), BF16),
            pltpu.VMEM((E * G, C, 2 * F), BF16),
            pltpu.VMEM((D, 2 * F), BF16),
            pltpu.VMEM((F, D), BF16),
            pltpu.VMEM((1, D), F32),
            pltpu.VMEM(rows, BF16), pltpu.VMEM(rows, BF16),
            pltpu.VMEM((E, G, C, D), BF16), pltpu.VMEM((E, G, C, D), BF16),
            pltpu.VMEM((E, C, 128), F32), pltpu.VMEM((E, C, 128), F32),
            pltpu.VMEM((T, padded), BF16), pltpu.VMEM((T, padded), BF16),
            pltpu.VMEM((E, G, C, D), BF16), pltpu.VMEM((E, G, C, D), BF16),
            pltpu.VMEM((E, G, C, D), BF16), pltpu.VMEM((E, G, C, D), BF16),
            pltpu.VMEM(rows, F32), pltpu.VMEM(rows, F32),
            pltpu.VMEM(rows, BF16), pltpu.VMEM(rows, BF16), pltpu.VMEM(rows, BF16),
            pltpu.VMEM(rows, BF16), pltpu.VMEM(rows, BF16),
            pltpu.VMEM((G * C, F), BF16),
            pltpu.VMEM((G * C, 2 * F), BF16),
            pltpu.VMEM((G * C, F), F32), pltpu.VMEM((G * C, 2 * F), F32),
            pltpu.VMEM((G * C, 2 * F), F32), pltpu.VMEM((G * C, 128), F32),
            pltpu.VMEM((C // halves, D), BF16),
            DMA((11,)), pltpu.SemaphoreType.REGULAR, DMA, DMA,
            DMA((2 * E - 1,)), DMA((2 * E - 1, N)), DMA, DMA,
            DMA((2, E, G - 1)), DMA((2, E, G - 1, N)), DMA((3,)), DMA((3,)),
            DMA((2, E, G - 1)), DMA((2, E - 1, G - 1, N)), DMA((2, G - 1)),
            DMA((E - 1,)), DMA((E - 1,)), DMA((E,)), DMA((E,)),
            DMA((E - 1,)), DMA((E - 1, halves)),
        ],
        compiler_params=pltpu.CompilerParams(
            collective_id=0, has_side_effects=True, vmem_limit_bytes=40 * 2**20
        ),
    )(*[
        pltpu.with_memory_space_constraint(a, pltpu.HBM)
        for a in (
            forward_ids.reshape(1, T),
            forward_gates.reshape(1, T),
            grad_ids.reshape(1, T),
            grad_gates.reshape(1, T),
            norm_gain,
            forward_in[0],
            grad_in[0],
            saved_input[0],
            saved_acts.reshape(E * G, C, 2 * F),
            weight_in[0],
            weight_out[0],
        )
    ])
    out_shape = jax.ShapeDtypeStruct((T, D), BF16)
    fwd, grad = pl.pallas_call(
        unsort,
        out_shape=(out_shape, out_shape),
        in_specs=[vmem] * 4,
        out_specs=(hbm, hbm),
        scratch_shapes=[pltpu.VMEM((2, T, D), BF16), DMA((2, UNSORT_STEPS))],
        compiler_params=pltpu.CompilerParams(vmem_limit_bytes=8 * 2**20),
    )(*[pltpu.with_memory_space_constraint(a, pltpu.VMEM) for a in arrived])
    return fwd[None], grad[None]


def solution(mesh):
    sources = mesh.shape["expert"]
    G = min(4, sources // 2)
    dims = (mesh.shape["pipe"], sources // G, G)
    placed = (
        P("pipe", "expert", None),
        P("pipe", "expert", None),
        P("pipe", "expert", None),
        P("pipe", "expert", None),
        P("pipe", "expert", None),
        P("pipe", "expert", None),
        P("pipe", "expert", None),
        P("pipe", "expert", None, None),
        P("pipe", None),
        P("expert", None, None),
        P("expert", None, None),
    )
    return jax.shard_map(
        functools.partial(on_device, dims),
        mesh=mesh,
        in_specs=placed,
        out_specs=(P("pipe", "expert", None), P("pipe", "expert", None)),
        check_vma=False,
    )
```

```python
import contextlib
import functools

import jax
import jax.numpy as jnp
from jax import lax
from jax.experimental import pallas as pl
from jax.experimental.pallas import tpu as pltpu
from jax.sharding import PartitionSpec as P

epsilon = 1e-06
F32 = jnp.float32
BF16 = jnp.bfloat16
MESH = pl.DeviceIdType.MESH


@contextlib.contextmanager
def stage(name):
    with jax.named_scope(name):
        pl.delay(1)
        yield


def tile_of(width, most):
    tile = most
    while width % tile:
        tile //= 2
    return tile


LAG = 2


def disp_rows(C):
    return 2 if C % 32 == 0 else 1


def columns_of(D, C):
    tile = tile_of(D, 512)
    tiles = D // tile
    width = tile * (-(-tiles // 4) if C % 32 == 0 else tiles)
    return [slice(d, min(d + width, D)) for d in range(0, D, width)]


def dot(a, b):
    return lax.dot_general(a, b, (((1,), (0,)), ((), ())), preferred_element_type=F32)


def dot_t(a, b):
    return lax.dot_general(a, b, (((1,), (1,)), ((), ())), preferred_element_type=F32)


def placing(ids_row, own, experts, capacity, padded):
    count = ids_row.shape[1]
    down = lax.broadcasted_iota(jnp.int32, (count, count), 0)
    across = lax.broadcasted_iota(jnp.int32, (count, count), 1)
    rel = ids_row - own
    rel = jnp.where(rel < 0, rel + experts, rel).astype(F32)
    spread = jnp.broadcast_to(rel, (count, count))
    column = jnp.sum(jnp.where(down == across, spread, 0.0), axis=1, keepdims=True)
    before = jnp.where((column == spread) & (down < across), 1.0, 0.0)
    rank = jnp.sum(before, axis=0, keepdims=True)
    slot = jnp.broadcast_to(rel * capacity + rank, (count, count))
    slot_column = jnp.sum(jnp.where(down == across, slot, 0.0), axis=1, keepdims=True)
    gather = jnp.where(down.astype(F32) == slot, 1.0, 0.0)
    wide = lax.broadcasted_iota(jnp.int32, (count, padded), 1).astype(F32)
    scatter = jnp.where(slot_column == wide, 1.0, 0.0).astype(BF16)
    return gather, scatter


def kernel(
    dims,
    fid_hbm, fgate_hbm, gid_hbm, ggate_hbm, gain_hbm,
    x_hbm, g_hbm, saved_hbm, acts_hbm, wi_hbm, wo_hbm,
    fin_f, fin_b, ur_f, ur_b,
    fid_ref, fgate_ref, gid_ref, ggate_ref, gain_ref,
    x_ref, g_ref, saved_ref, acts_ref, wi, wo, gain_f,
    xs_f, xs_b, rx_f, rx_b, gs_f, rg_f, us_f, us_b,
    part_f, part_b, rpart_f, rpart_b, own_f, own_b,
    mv, pb, ret_b, th, srt, hidden_ref, joined, sum_b, both_b, sum_f, square_f,
    via, w_sem, ready_sem, side_sem, via_s, via_r,
    disp_s, disp_r, gate_s, gate_r, relay_s, relay_r, perm_s, perm_r, red_s, red_r, near_r,
    move_s, move_r, out_s, out_r, ret_s, ret_r,
):
    pipes, E, G = dims
    s = lax.axis_index("pipe")
    position = lax.axis_index("expert")
    e = position // G
    g = position % G
    C, D = xs_f.shape[1:]
    T = x_ref.shape[0]
    F = wo.shape[0]

    def dev(hop, k, j):
        return (
            (s + hop + pipes) % pipes,
            ((e + k + E) % E) * G + (g + j + G) % G,
        )

    near = [dev(0, k, 0) for k in range(1, E)] + [dev(0, 0, j) for j in range(1, G)]
    beside = [dev(0, k, 0) for k in range(1, E)]
    following, previous = [dev(1, 0, 0)], [dev(-1, 0, 0)]
    first, last = s == 0, s == pipes - 1

    def greet(sem, peers):
        for peer in peers:
            pl.semaphore_signal(sem, inc=1, device_id=peer, device_id_type=MESH)

    barrier = pltpu.get_barrier_semaphore()
    greet(barrier, near)
    greet(barrier, previous)
    pl.when(s != pipes - 1)(lambda: greet(barrier, following))
    pairs = (
        (gid_hbm, gid_ref), (g_hbm, g_ref), (fid_hbm, fid_ref), (fgate_hbm, fgate_ref),
        (ggate_hbm, ggate_ref), (gain_hbm, gain_ref), (x_hbm, x_ref), (saved_hbm, saved_ref), (acts_hbm, acts_ref),
        (wo_hbm, wo), (wi_hbm, wi),
    )
    loads = [
        pltpu.make_async_copy(source, held, w_sem.at[i]) for i, (source, held) in enumerate(pairs)
    ]
    for load in loads:
        load.start()
    load_gid, load_g, *load_small, load_x, load_saved, load_acts, load_wo, load_wi = loads

    def remote(src, dst, send, recv, target):
        copy = pltpu.make_async_remote_copy(
            src_ref=src, dst_ref=dst, send_sem=send, recv_sem=recv,
            device_id=target, device_id_type=MESH,
        )
        copy.start()
        return copy

    def whole(src, dst, send, recv, target=None):
        return pltpu.make_async_remote_copy(
            src_ref=src, dst_ref=dst, send_sem=send, recv_sem=recv,
            device_id=dev(1, 0, 0) if target is None else target, device_id_type=MESH,
        )

    xs, rx = (xs_f, xs_b), (rx_f, rx_b)
    part, rpart = (part_f, part_b), (rpart_f, rpart_b)
    own = (own_f, own_b)
    halves = disp_rows(C)
    half = C // halves
    tile_d = tile_of(D, 512)
    chunks = columns_of(D, C)
    count = len(chunks)
    others = range(1, E)

    def flat(rows):
        if C % 16:
            return rows.astype(F32).reshape(-1, rows.shape[-1]).astype(BF16)
        return rows.reshape(-1, rows.shape[-1])

    relay, reduce = {}, {}

    def outgoing(b, k, c):
        return pltpu.make_async_remote_copy(
            src_ref=xs[b].at[k, :, chunks[c]], dst_ref=rx[b].at[k, 0, :, chunks[c]],
            send_sem=disp_s.at[b * (E - 1) + k], recv_sem=disp_r.at[b * (E - 1) + k, c],
            device_id=dev(1 - b, k, 0), device_id_type=MESH,
        )

    def share(b, k, c, source):
        for j in range(1, G):
            relay[b, k, j, c] = remote(
                source, rx[b].at[k, j, :, chunks[c]],
                relay_s.at[b, k, j - 1], relay_r.at[b, k, j - 1, c], dev(0, 0, j),
            )

    def pass_on(b, k, c):
        with jax.named_scope(f"pass_{b}_{k}_{c}"):
            outgoing(b, k, c).wait_recv()
            share(b, k, c, rx[b].at[k, 0, :, chunks[c]])

    def arrived(b, k, c):
        with jax.named_scope(f"arr_{b}_{k}_{c}"):
            for j in range(1, G):
                relay[b, k, j, c].wait_recv()

    def put_part(b, k, rows, columns):
        rows = rows.reshape(G, C, rows.shape[-1])
        own[b][k, :, columns] = rows[0]
        for j in range(1, G):
            part[b][k, j, :, columns] = rows[G - j].astype(BF16)

    def send_part(b, k, c):
        for j in range(1, G):
            reduce[b, k, j, c] = remote(
                part[b].at[k, j, :, chunks[c]], rpart[b].at[k, j, :, chunks[c]],
                red_s.at[b, k, j - 1], landed(b, k, j, c), dev(0, 0, j),
            )

    def landed(b, k, j, c):
        return red_r.at[b, k - 1, j - 1, c] if k else near_r.at[b, j - 1]

    def wait_near(b):
        for j in range(1, G):
            whole(
                part[b].at[0, j], rpart[b].at[0, j], red_s.at[b, 0, j - 1], near_r.at[b, j - 1]
            ).wait_recv()

    def summed(b, k, c):
        total = own[b][k, :, chunks[c]]
        for j in range(1, G):
            if k:
                with jax.named_scope(f"red_{b}_{k}_{c}"):
                    reduce[b, k, j, c].wait_recv()
            total = total + rpart[b][k, j, :, chunks[c]].astype(F32)
        return total

    def backward_first(k, c):
        arrived(1, k, c)
        grad = dot_t(flat(rx_b[k, :, :, chunks[c]]), wo[:, chunks[c]])
        sum_b[...] = grad if c == 0 else sum_b[...] + grad

    def backward_hidden(k):
        for j in range(G):
            source = ((e - k + E) % E) * G + (g - j + G) % G
            rows = slice(j * C, (j + 1) * C)
            grad = sum_b[rows, :]
            acts = acts_ref[source].astype(F32)
            gate_act, up_act = acts[:, :F], acts[:, F:]
            squashed = jax.nn.sigmoid(gate_act)
            gate_grad = grad * up_act * squashed * (1.0 + gate_act * (1.0 - squashed))
            both_b[rows, :F] = gate_grad
            both_b[rows, F:] = grad * gate_act * squashed
        joined[...] = both_b[...].astype(BF16)

    def backward_second(k, c):
        for d in range(chunks[c].start, chunks[c].stop, tile_d):
            columns = slice(d, d + tile_d)
            put_part(1, k, dot_t(joined[...], wi[columns, :]), columns)
        send_part(1, k, c)

    def send_back(k, c, h):
        rows = slice(h * half, (h + 1) * half)
        remote(
            pb.at[k, rows, chunks[c]], ret_b.at[k, rows, chunks[c]],
            ret_s.at[k - 1], ret_r.at[k - 1, h], dev(0, -k, 0),
        )

    def backward_return(k, c):
        pb[k, :, chunks[c]] = summed(1, k, c).astype(BF16)
        send_back(k, c, 0)

    def backward_end(k, h):
        low, high = h * half, (h + 1) * half
        if k:
            with stage(f"ret_{k}_{h}"):
                rows = slice(low, high)
                whole(
                    pb.at[k, rows], ret_b.at[k, rows], ret_s.at[k - 1], ret_r.at[k - 1, h]
                ).wait_recv()
            pulled = ret_b[k, low:high].astype(F32)
        else:
            pulled = own_b[0, low:high]
            if h == 0:
                with jax.named_scope("red_b0"):
                    wait_near(1)
            for j in range(1, G):
                pulled = pulled + rpart_b[0, j, low:high].astype(F32)
        weighted = gates_b[k * C + low : k * C + high] * pulled * gain_ref[...]
        before = srt[k, low:high].astype(F32)
        inverse = lax.rsqrt(jnp.mean(before * before, axis=-1, keepdims=True) + epsilon)
        unit = before * inverse
        inner = jnp.mean(weighted * unit, axis=-1, keepdims=True)
        th[k, low:high] = (
            xs_b[k, low:high].astype(F32) + inverse * (weighted - unit * inner)
        ).astype(BF16)

    def send_end(k, h):
        rows = slice(h * half, (h + 1) * half)
        remote(th.at[k, rows], fin_b.at[k, rows], out_s.at[k], out_r.at[k], dev(-1, 0, 0))

    detour = pipes > 2 and halves > 1
    low_rows = slice(half, 2 * half)

    cut = tile_d * ((D * 5 // 7) // tile_d)
    by, direct = slice(0, cut), slice(cut, D)

    def by_way(target):
        return whole(via.at[:, by], fin_b.at[0, low_rows, by], via_s, out_r.at[0], target)

    def send_near(h):
        if h != 1 or not detour:
            send_end(0, h)
            return
        pl.when(s != 1)(lambda: send_end(0, h))

        @pl.when(s == 1)
        def _():
            remote(th.at[0, low_rows, by], via.at[:, by], out_s.at[0], via_r, dev(1, 0, 0))
            remote(
                th.at[0, low_rows, direct], fin_b.at[0, low_rows, direct],
                out_s.at[0], out_r.at[0], dev(-1, 0, 0),
            )

    def forward_via():
        if detour:
            @pl.when(s == 2)
            def _():
                whole(th.at[0, low_rows, by], via.at[:, by], out_s.at[0], via_r).wait_recv()
                by_way(dev(-2, 0, 0)).start()

    def forward_first(k, c):
        arrived(0, k, c)
        rows = rx_f[k, :, :, chunks[c]].astype(F32).reshape(G * C, -1)
        lanes = [rows[:, i : i + 128] for i in range(0, rows.shape[1], 128)]
        square = sum(lane * lane for lane in lanes)
        square_f[...] = square if c == 0 else square_f[...] + square
        scaled = (rows * gain_f[:, chunks[c]]).astype(BF16)
        for f in range(0, 2 * F, tile_f):
            hidden = dot(scaled, wi[chunks[c], f : f + tile_f])
            columns = slice(f, f + tile_f)
            sum_f[:, columns] = hidden if c == 0 else sum_f[:, columns] + hidden

    def forward_hidden():
        mean = jnp.sum(square_f[...], axis=-1, keepdims=True) * (1.0 / D)
        inverse = lax.rsqrt(mean + epsilon)
        for f in range(0, F, tile_f):
            gate = sum_f[:, f : f + tile_f] * inverse
            up = sum_f[:, F + f : F + f + tile_f] * inverse
            hidden_ref[:, f : f + tile_f] = (jax.nn.silu(gate) * up).astype(BF16)

    def forward_second(k, c):
        for d in range(chunks[c].start, chunks[c].stop, tile_d):
            columns = slice(d, d + tile_d)
            put_part(0, k, dot(hidden_ref[...], wo[:, columns]), columns)
        send_part(0, k, c)

    def forward_end(k, c):
        total = summed(0, k, c)
        moved = rx_f[k, 0, :, chunks[c]].astype(F32) + rg_f[k][:, :1] * total
        if k == 0:
            fin_f[0, :, chunks[c]] = moved.astype(BF16)
            return
        mv[k, :, chunks[c]] = moved.astype(BF16)
        remote(
            mv.at[k, :, chunks[c]], fin_f.at[k, :, chunks[c]],
            move_s.at[k - 1], move_r.at[k - 1], dev(0, -k, 0),
        )

    tile_f = tile_of(F, 256)
    with jax.named_scope("w_small"):
        for load in (load_gid, *load_small):
            load.wait()
    gather_f, scatter_f = placing(fid_ref[...], e, E, C, us_f.shape[1])
    gather_b, scatter_b = placing(gid_ref[...], e, E, C, us_b.shape[1])
    gather_f_rows, gather_b_rows = gather_f.astype(BF16), gather_b.astype(BF16)
    us_b[...] = scatter_b
    us_f[...] = scatter_f
    gates_b = jnp.sum(gather_b * ggate_ref[...], axis=1, keepdims=True)
    gates_f = jnp.sum(gather_f * fgate_ref[...], axis=1, keepdims=True)
    gs_f[...] = jnp.broadcast_to(gates_f, (T, gs_f.shape[2])).reshape(gs_f.shape)
    early = count // 2
    with jax.named_scope("w_x"):
        load_x.wait()
    for c in range(count):
        xs_f[:, :, chunks[c]] = (
            dot(gather_f_rows, x_ref[:, chunks[c]]).reshape(E, C, -1).astype(BF16)
        )
    arrivals = len(near) + 1 + (s + pipes - 1) // pipes

    def send_forward(order):
        for k, c in order:
            outgoing(0, k, c).start()

    far = [(k, c) for k in others for c in range(count)]
    own_rows = [(0, c) for c in range(count)]

    @pl.when(last)
    def _():
        pl.semaphore_wait(barrier, arrivals)
        send_forward(own_rows[-1:])

    with jax.named_scope("w_g"):
        load_g.wait()
    for c in range(count):
        rows = dot(gather_b_rows, g_ref[:, chunks[c]]).reshape(E, C, -1).astype(BF16)
        xs_b[:, :, chunks[c]] = rows
        rx_b[0, 0, :, chunks[c]] = rows[0]
    with jax.named_scope("w_bar"):
        pl.when(s != pipes - 1)(lambda: pl.semaphore_wait(barrier, arrivals))
    gain_copy = remote(gain_ref, gain_f, perm_s.at[2], perm_r.at[2], dev(1, 0, 0))
    remote(gs_f.at[0], rg_f.at[0], gate_s, gate_r, dev(1, 0, 0))
    perm_f = remote(us_f, ur_f, perm_s.at[0], perm_r.at[0], dev(1, 0, 0))

    greet(side_sem, beside)
    pl.when(s != pipes - 1)(lambda: send_forward(own_rows))
    for c in range(count):
        for k in others:
            outgoing(1, k, c).start()
    for c in range(count):
        share(1, 0, c, xs_b.at[0, :, chunks[c]])
    pl.when(last)(lambda: greet(ready_sem, following))
    with jax.named_scope("w_saved"):
        load_saved.wait()
    srt[...] = dot(gather_b_rows, saved_ref[...]).reshape(E, C, D).astype(BF16)
    with stage("w_side"):
        pl.semaphore_wait(side_sem, len(beside))
    for k in others:
        remote(gs_f.at[k], rg_f.at[k], gate_s, gate_r, dev(1, k, 0))
    send_forward(far)
    pl.when(last)(lambda: send_forward(own_rows[:-1]))

    with jax.named_scope("w_wo"):
        load_wo.wait()
        load_acts.wait()
    with stage("b1_0"):
        for c in range(count):
            backward_first(0, c)
        backward_hidden(0)
    with jax.named_scope("w_wi"):
        load_wi.wait()

    def near_end():
        whole(us_b, ur_b, perm_s.at[1], perm_r.at[1], dev(-1, 0, 0)).start()
        for h in range(halves):
            send_near(h)

    def last_ends():
        for k in others:
            for h in range(1, halves):
                with stage(f"bend1_{h}"):
                    backward_end(k, h)
                    send_end(k, h)

    for c in range(count):
        with stage(f"b2_0_{c}"):
            backward_second(0, c)
        if 1 <= c <= early:
            for k in others:
                pass_on(1, k, c - 1)
    for c in range(early):
        with stage(f"b1_1a{c}"):
            backward_first(1, c)
        if c == 0:
            for k in others:
                for i in range(early, count - 1):
                    pass_on(1, k, i)
    for k in others:
        pass_on(1, k, count - 1)
    with stage("bend0"):
        for h in range(halves):
            backward_end(0, h)
    for k in others:
        with stage("b1_1b"):
            for c in range(early if k == 1 else 0, count):
                backward_first(k, c)
            backward_hidden(k)
        for c in range(count):
            with stage(f"b2_1_{c}"):
                backward_second(k, c)
            if k == 1 and c == min(2, count - 1):
                pl.when(s != 0)(near_end)
            if k == E - 1 and c >= early > 0:
                for other in others:
                    pass_on(0, other, c - early)
            if c >= 1:
                with stage(f"bret_{c - 1}"):
                    backward_return(k, c - 1)
        if k == E - 1:
            for other in others:
                for c in range(early, count - 1):
                    pass_on(0, other, c)
        with stage(f"bret_{count - 1}"):
            backward_return(k, count - 1)
        if k == E - 1:
            for other in others:
                pass_on(0, other, count - 1)
        for h in range(1, halves):
            for c in range(count):
                send_back(k, c, h)
    with jax.named_scope("w_gain"):
        gain_copy.wait_recv()
    with jax.named_scope("w_prev"):
        pl.when(first)(lambda: pl.semaphore_wait(ready_sem, 1))
        pl.when(first)(near_end)
    with jax.named_scope("w_gate"):
        whole(gs_f, rg_f, gate_s, gate_r).wait_recv()
    for k in others:
        for c in range(count):
            with stage(f"f1_1_{c}"):
                forward_first(k, c)
        with stage("fh_1"):
            forward_hidden()
        if k == 1:
            with jax.named_scope("w_via"):
                forward_via()
        for c in range(count):
            with stage(f"f2_1_{c}"):
                forward_second(k, c)
            if c == max(LAG, count - 2) or count == 1:
                with stage("bend1_0"):
                    backward_end(k, 0)
                    send_end(k, 0)
            if c >= LAG:
                with stage(f"fend_1_{c - LAG}"):
                    forward_end(k, c - LAG)
        if k == E - 1:
            for c in range(count):
                pass_on(0, 0, c)
        for c in range(max(count - LAG, 0), count):
            with stage(f"fend_1_{c}"):
                forward_end(k, c)
    for c in range(count):
        with stage(f"f1_0_{c}"):
            forward_first(0, c)
        if c == early - 1:
            last_ends()
    with stage("fh_0"):
        forward_hidden()
    with stage("f2_0"):
        for c in range(count):
            forward_second(0, c)
    if early == 0:
        last_ends()
    with stage("fend0"):
        wait_near(0)
        for c in range(count):
            forward_end(0, c)

    with jax.named_scope("w_perm"):
        perm_f.wait_recv()
        whole(us_b, ur_b, perm_s.at[1], perm_r.at[1]).wait_recv()
    for k in others:
        with jax.named_scope("w_move"):
            whole(mv.at[k], fin_f.at[k], move_s.at[k - 1], move_r.at[k - 1]).wait_recv()
    for k in range(E):
        with jax.named_scope(f"w_out{k}"):
            whole(th.at[k], fin_b.at[k], out_s.at[k], out_r.at[k]).wait_recv()
    with jax.named_scope("w_sends"):
        for b in range(2):
            for k in range(b, E):
                i = b * (E - 1) + k
                whole(xs[b].at[k], rx[b].at[k, 0], disp_s.at[i], disp_r.at[i, 0]).wait_send()
            for k in range(E):
                for j in range(1, G):
                    i = (b, k, j - 1)
                    whole(
                        rx[b].at[k, 0], rx[b].at[k, j], relay_s.at[i], relay_r.at[(*i, 0)]
                    ).wait_send()
                    whole(part[b].at[k, j], rpart[b].at[k, j], red_s.at[i], near_r.at[b, j - 1]).wait_send()
        for k in others:
            whole(pb.at[k], ret_b.at[k], ret_s.at[k - 1], ret_r.at[k - 1, 0]).wait_send()
            whole(mv.at[k], fin_f.at[k], move_s.at[k - 1], move_r.at[k - 1]).wait_send()
        for k in range(E):
            whole(th.at[k], fin_b.at[k], out_s.at[k], out_r.at[k]).wait_send()
        whole(gs_f, rg_f, gate_s, gate_r).wait_send()
        if detour:
            pl.when(s == 2)(lambda: by_way(dev(-2, 0, 0)).wait_send())
        for copy in (gain_copy, perm_f, whole(us_b, ur_b, perm_s.at[1], perm_r.at[1])):
            copy.wait_send()


UNSORT_STEPS = 2


def unsort(fin_f, fin_b, ur_f, ur_b, fout_hbm, gout_hbm, held, sems):
    T, D = fout_hbm.shape
    width = D // UNSORT_STEPS
    copies = []
    for i, (fin, ur, out) in enumerate(((fin_f, ur_f, fout_hbm), (fin_b, ur_b, gout_hbm))):
        for c in range(UNSORT_STEPS):
            columns = pl.ds(c * width, width)
            rows = fin[:, :, columns].astype(F32).reshape(T, width).astype(BF16)
            held[i, :, columns] = dot(ur[:, :T], rows).astype(BF16)
            copy = pltpu.make_async_copy(held.at[i, :, columns], out.at[:, columns], sems.at[i, c])
            copy.start()
            copies.append(copy)
    for copy in copies:
        copy.wait()


def on_device(
    dims,
    forward_in,
    forward_ids,
    forward_gates,
    grad_in,
    grad_ids,
    grad_gates,
    saved_input,
    saved_acts,
    norm_gain,
    weight_in,
    weight_out,
):
    pipes, E, G = dims
    T, D = forward_in.shape[1:]
    F = weight_out.shape[1]
    C = T // E
    padded = -(-T // 128) * 128
    DMA = pltpu.SemaphoreType.DMA
    rows = (E, C, D)
    vmem = pl.BlockSpec(memory_space=pltpu.VMEM)
    hbm = pl.BlockSpec(memory_space=pl.ANY)
    sorted_rows = jax.ShapeDtypeStruct(rows, BF16)
    order = jax.ShapeDtypeStruct((T, padded), BF16)
    halves, N = disp_rows(C), len(columns_of(D, C))
    arrived = pl.pallas_call(
        functools.partial(kernel, dims),
        out_shape=(pltpu.VMEM(rows, BF16), pltpu.VMEM(rows, BF16), pltpu.VMEM((T, padded), BF16), pltpu.VMEM((T, padded), BF16)),
        in_specs=[hbm] * 11,
        out_specs=(vmem, vmem, vmem, vmem),
        scratch_shapes=[
            pltpu.VMEM((1, T), jnp.int32), pltpu.VMEM((1, T), F32),
            pltpu.VMEM((1, T), jnp.int32), pltpu.VMEM((1, T), F32),
            pltpu.VMEM((1, D), F32),
            pltpu.VMEM((T, D), BF16), pltpu.VMEM((T, D), BF16), pltpu.VMEM((T, D), BF16),
            pltpu.VMEM((E * G, C, 2 * F), BF16),
            pltpu.VMEM((D, 2 * F), BF16),
            pltpu.VMEM((F, D), BF16),
            pltpu.VMEM((1, D), F32),
            pltpu.VMEM(rows, BF16), pltpu.VMEM(rows, BF16),
            pltpu.VMEM((E, G, C, D), BF16), pltpu.VMEM((E, G, C, D), BF16),
            pltpu.VMEM((E, C, 128), F32), pltpu.VMEM((E, C, 128), F32),
            pltpu.VMEM((T, padded), BF16), pltpu.VMEM((T, padded), BF16),
            pltpu.VMEM((E, G, C, D), BF16), pltpu.VMEM((E, G, C, D), BF16),
            pltpu.VMEM((E, G, C, D), BF16), pltpu.VMEM((E, G, C, D), BF16),
            pltpu.VMEM(rows, F32), pltpu.VMEM(rows, F32),
            pltpu.VMEM(rows, BF16), pltpu.VMEM(rows, BF16), pltpu.VMEM(rows, BF16),
            pltpu.VMEM(rows, BF16), pltpu.VMEM(rows, BF16),
            pltpu.VMEM((G * C, F), BF16),
            pltpu.VMEM((G * C, 2 * F), BF16),
            pltpu.VMEM((G * C, F), F32), pltpu.VMEM((G * C, 2 * F), F32),
            pltpu.VMEM((G * C, 2 * F), F32), pltpu.VMEM((G * C, 128), F32),
            pltpu.VMEM((C // halves, D), BF16),
            DMA((11,)), pltpu.SemaphoreType.REGULAR, pltpu.SemaphoreType.REGULAR, DMA, DMA,
            DMA((2 * E - 1,)), DMA((2 * E - 1, N)), DMA, DMA,
            DMA((2, E, G - 1)), DMA((2, E, G - 1, N)), DMA((3,)), DMA((3,)),
            DMA((2, E, G - 1)), DMA((2, E - 1, G - 1, N)), DMA((2, G - 1)),
            DMA((E - 1,)), DMA((E - 1,)), DMA((E,)), DMA((E,)),
            DMA((E - 1,)), DMA((E - 1, halves)),
        ],
        compiler_params=pltpu.CompilerParams(
            collective_id=0, has_side_effects=True, vmem_limit_bytes=40 * 2**20
        ),
    )(*[
        pltpu.with_memory_space_constraint(a, pltpu.HBM)
        for a in (
            forward_ids.reshape(1, T),
            forward_gates.reshape(1, T),
            grad_ids.reshape(1, T),
            grad_gates.reshape(1, T),
            norm_gain,
            forward_in[0],
            grad_in[0],
            saved_input[0],
            saved_acts.reshape(E * G, C, 2 * F),
            weight_in[0],
            weight_out[0],
        )
    ])
    out_shape = jax.ShapeDtypeStruct((T, D), BF16)
    fwd, grad = pl.pallas_call(
        unsort,
        out_shape=(out_shape, out_shape),
        in_specs=[vmem] * 4,
        out_specs=(hbm, hbm),
        scratch_shapes=[pltpu.VMEM((2, T, D), BF16), DMA((2, UNSORT_STEPS))],
        compiler_params=pltpu.CompilerParams(vmem_limit_bytes=8 * 2**20),
    )(*[pltpu.with_memory_space_constraint(a, pltpu.VMEM) for a in arrived])
    return fwd[None], grad[None]


def solution(mesh):
    sources = mesh.shape["expert"]
    G = min(4, sources // 2)
    dims = (mesh.shape["pipe"], sources // G, G)
    placed = (
        P("pipe", "expert", None),
        P("pipe", "expert", None),
        P("pipe", "expert", None),
        P("pipe", "expert", None),
        P("pipe", "expert", None),
        P("pipe", "expert", None),
        P("pipe", "expert", None),
        P("pipe", "expert", None, None),
        P("pipe", None),
        P("expert", None, None),
        P("expert", None, None),
    )
    return jax.shard_map(
        functools.partial(on_device, dims),
        mesh=mesh,
        in_specs=placed,
        out_specs=(P("pipe", "expert", None), P("pipe", "expert", None)),
        check_vma=False,
    )
```

```python
import contextlib
import functools

import jax
import jax.numpy as jnp
from jax import lax
from jax.experimental import pallas as pl
from jax.experimental.pallas import tpu as pltpu
from jax.sharding import PartitionSpec as P

epsilon = 1e-06
F32 = jnp.float32
BF16 = jnp.bfloat16
MESH = pl.DeviceIdType.MESH


@contextlib.contextmanager
def stage(name):
    with jax.named_scope(name):
        pl.delay(1)
        yield


def tile_of(width, most):
    tile = most
    while width % tile:
        tile //= 2
    return tile


LAG = 2


def disp_rows(C):
    return 2 if C % 32 == 0 else 1


def columns_of(D, C):
    tile = tile_of(D, 512)
    tiles = D // tile
    width = tile * (-(-tiles // 4) if C % 32 == 0 else tiles)
    return [slice(d, min(d + width, D)) for d in range(0, D, width)]


def dot(a, b):
    return lax.dot_general(a, b, (((1,), (0,)), ((), ())), preferred_element_type=F32)


def dot_t(a, b):
    return lax.dot_general(a, b, (((1,), (1,)), ((), ())), preferred_element_type=F32)


def placing(ids_row, own, experts, capacity, padded):
    count = ids_row.shape[1]
    down = lax.broadcasted_iota(jnp.int32, (count, count), 0)
    across = lax.broadcasted_iota(jnp.int32, (count, count), 1)
    rel = ids_row - own
    rel = jnp.where(rel < 0, rel + experts, rel).astype(F32)
    spread = jnp.broadcast_to(rel, (count, count))
    column = jnp.sum(jnp.where(down == across, spread, 0.0), axis=1, keepdims=True)
    before = jnp.where((column == spread) & (down < across), 1.0, 0.0)
    rank = jnp.sum(before, axis=0, keepdims=True)
    slot = jnp.broadcast_to(rel * capacity + rank, (count, count))
    slot_column = jnp.sum(jnp.where(down == across, slot, 0.0), axis=1, keepdims=True)
    gather = jnp.where(down.astype(F32) == slot, 1.0, 0.0)
    wide = lax.broadcasted_iota(jnp.int32, (count, padded), 1).astype(F32)
    scatter = jnp.where(slot_column == wide, 1.0, 0.0).astype(BF16)
    return gather, scatter


def kernel(
    dims,
    fid_hbm, fgate_hbm, gid_hbm, ggate_hbm, gain_hbm,
    x_hbm, g_hbm, saved_hbm, acts_hbm, wi_hbm, wo_hbm,
    fin_f, fin_b, ur_f, ur_b,
    fid_ref, fgate_ref, gid_ref, ggate_ref, gain_ref,
    x_ref, g_ref, saved_ref, acts_ref, wi, wo, gain_f,
    xs_f, xs_b, rx_f, rx_b, gs_f, rg_f, us_f, us_b,
    part_f, part_b, rpart_f, rpart_b, own_f, own_b,
    mv, pb, ret_b, th, srt, hidden_ref, joined, sum_b, both_b, sum_f, square_f,
    via, w_sem, ready_sem, side_sem, via_s, via_r,
    disp_s, disp_r, gate_s, gate_r, relay_s, relay_r, perm_s, perm_r, red_s, red_r, near_r,
    row_r, same_r,
    move_s, move_r, out_s, out_r, ret_s, ret_r,
):
    pipes, E, G = dims
    s = lax.axis_index("pipe")
    position = lax.axis_index("expert")
    e = position // G
    g = position % G
    C, D = xs_f.shape[1:]
    T = x_ref.shape[0]
    F = wo.shape[0]

    def dev(hop, k, j):
        return (
            (s + hop + pipes) % pipes,
            ((e + k + E) % E) * G + (g + j + G) % G,
        )

    near = [dev(0, k, 0) for k in range(1, E)] + [dev(0, 0, j) for j in range(1, G)]
    beside = [dev(0, k, 0) for k in range(1, E)]
    following, previous = [dev(1, 0, 0)], [dev(-1, 0, 0)]
    first, last = s == 0, s == pipes - 1

    def greet(sem, peers):
        for peer in peers:
            pl.semaphore_signal(sem, inc=1, device_id=peer, device_id_type=MESH)

    barrier = pltpu.get_barrier_semaphore()
    greet(barrier, near)
    greet(barrier, previous)
    pl.when(s != pipes - 1)(lambda: greet(barrier, following))
    pairs = (
        (gid_hbm, gid_ref), (g_hbm, g_ref), (fid_hbm, fid_ref), (fgate_hbm, fgate_ref),
        (ggate_hbm, ggate_ref), (gain_hbm, gain_ref), (x_hbm, x_ref), (saved_hbm, saved_ref), (acts_hbm, acts_ref),
        (wo_hbm, wo), (wi_hbm, wi),
    )
    loads = [
        pltpu.make_async_copy(source, held, w_sem.at[i]) for i, (source, held) in enumerate(pairs)
    ]
    for load in loads:
        load.start()
    load_gid, load_g, *load_small, load_x, load_saved, load_acts, load_wo, load_wi = loads

    def remote(src, dst, send, recv, target):
        copy = pltpu.make_async_remote_copy(
            src_ref=src, dst_ref=dst, send_sem=send, recv_sem=recv,
            device_id=target, device_id_type=MESH,
        )
        copy.start()
        return copy

    def whole(src, dst, send, recv, target=None):
        return pltpu.make_async_remote_copy(
            src_ref=src, dst_ref=dst, send_sem=send, recv_sem=recv,
            device_id=dev(1, 0, 0) if target is None else target, device_id_type=MESH,
        )

    xs, rx = (xs_f, xs_b), (rx_f, rx_b)
    part, rpart = (part_f, part_b), (rpart_f, rpart_b)
    own = (own_f, own_b)
    halves = disp_rows(C)
    half = C // halves
    tile_d = tile_of(D, 512)
    chunks = columns_of(D, C)
    count = len(chunks)
    others = range(1, E)

    def flat(rows):
        if C % 16:
            return rows.astype(F32).reshape(-1, rows.shape[-1]).astype(BF16)
        return rows.reshape(-1, rows.shape[-1])

    relay, reduce = {}, {}

    def outgoing(b, k, c):
        return pltpu.make_async_remote_copy(
            src_ref=xs[b].at[k, :, chunks[c]], dst_ref=rx[b].at[k, 0, :, chunks[c]],
            send_sem=disp_s.at[b], recv_sem=disp_r.at[b, k - 1, c] if k else row_r,
            device_id=dev(1 - b, k, 0), device_id_type=MESH,
        )

    def share(b, k, c, source):
        for j in range(1, G):
            relay[b, k, j, c] = remote(
                source, rx[b].at[k, j, :, chunks[c]],
                relay_s.at[b, j - 1], relay_r.at[b, k - 1, j - 1, c], dev(0, 0, j),
            )

    def same(b, j, source):
        return whole(
            source, rx[b].at[0, j], relay_s.at[b, j - 1], same_r.at[b, j - 1], dev(0, 0, j)
        )

    def pass_on(b, k, c):
        with jax.named_scope(f"pass_{b}_{k}_{c}"):
            outgoing(b, k, c).wait_recv()
            share(b, k, c, rx[b].at[k, 0, :, chunks[c]])

    def arrived(b, k, c):
        with jax.named_scope(f"arr_{b}_{k}_{c}"):
            for j in range(1, G):
                if k:
                    relay[b, k, j, c].wait_recv()
                elif c == 0:
                    same(b, j, xs[b].at[0]).wait_recv()

    def put_part(b, k, rows, columns):
        rows = rows.reshape(G, C, rows.shape[-1])
        own[b][k, :, columns] = rows[0]
        for j in range(1, G):
            part[b][k, j, :, columns] = rows[G - j].astype(BF16)

    def send_part(b, k, c):
        for j in range(1, G):
            reduce[b, k, j, c] = remote(
                part[b].at[k, j, :, chunks[c]], rpart[b].at[k, j, :, chunks[c]],
                red_s.at[b, j - 1], landed(b, k, j, c), dev(0, 0, j),
            )

    def landed(b, k, j, c):
        return red_r.at[b, k - 1, j - 1, c] if k else near_r.at[b, j - 1]

    def wait_near(b):
        for j in range(1, G):
            whole(
                part[b].at[0, j], rpart[b].at[0, j], red_s.at[b, j - 1], near_r.at[b, j - 1]
            ).wait_recv()

    def summed(b, k, c):
        total = own[b][k, :, chunks[c]]
        for j in range(1, G):
            if k:
                with jax.named_scope(f"red_{b}_{k}_{c}"):
                    reduce[b, k, j, c].wait_recv()
            total = total + rpart[b][k, j, :, chunks[c]].astype(F32)
        return total

    def backward_first(k, c):
        arrived(1, k, c)
        grad = dot_t(flat(rx_b[k, :, :, chunks[c]]), wo[:, chunks[c]])
        sum_b[...] = grad if c == 0 else sum_b[...] + grad

    def backward_hidden(k):
        for j in range(G):
            source = ((e - k + E) % E) * G + (g - j + G) % G
            rows = slice(j * C, (j + 1) * C)
            grad = sum_b[rows, :]
            acts = acts_ref[source].astype(F32)
            gate_act, up_act = acts[:, :F], acts[:, F:]
            squashed = jax.nn.sigmoid(gate_act)
            gate_grad = grad * up_act * squashed * (1.0 + gate_act * (1.0 - squashed))
            both_b[rows, :F] = gate_grad
            both_b[rows, F:] = grad * gate_act * squashed
        joined[...] = both_b[...].astype(BF16)

    def backward_second(k, c):
        for d in range(chunks[c].start, chunks[c].stop, tile_d):
            columns = slice(d, d + tile_d)
            put_part(1, k, dot_t(joined[...], wi[columns, :]), columns)
        send_part(1, k, c)

    def send_back(k, c, h):
        rows = slice(h * half, (h + 1) * half)
        remote(
            pb.at[k, rows, chunks[c]], ret_b.at[k, rows, chunks[c]],
            ret_s.at[k - 1], ret_r.at[k - 1, h], dev(0, -k, 0),
        )

    def backward_return(k, c):
        pb[k, :, chunks[c]] = summed(1, k, c).astype(BF16)
        send_back(k, c, 0)

    def backward_end(k, h):
        low, high = h * half, (h + 1) * half
        if k:
            with stage(f"ret_{k}_{h}"):
                rows = slice(low, high)
                whole(
                    pb.at[k, rows], ret_b.at[k, rows], ret_s.at[k - 1], ret_r.at[k - 1, h]
                ).wait_recv()
            pulled = ret_b[k, low:high].astype(F32)
        else:
            pulled = own_b[0, low:high]
            if h == 0:
                with jax.named_scope("red_b0"):
                    wait_near(1)
            for j in range(1, G):
                pulled = pulled + rpart_b[0, j, low:high].astype(F32)
        weighted = gates_b[k * C + low : k * C + high] * pulled * gain_ref[...]
        before = srt[k, low:high].astype(F32)
        inverse = lax.rsqrt(jnp.mean(before * before, axis=-1, keepdims=True) + epsilon)
        unit = before * inverse
        inner = jnp.mean(weighted * unit, axis=-1, keepdims=True)
        th[k, low:high] = (
            xs_b[k, low:high].astype(F32) + inverse * (weighted - unit * inner)
        ).astype(BF16)

    def send_end(k, h):
        rows = slice(h * half, (h + 1) * half)
        remote(th.at[k, rows], fin_b.at[k, rows], out_s, out_r, dev(-1, 0, 0))

    detour = pipes > 2 and halves > 1
    low_rows = slice(half, 2 * half)

    cut = tile_d * ((D * 5 // 7) // tile_d)
    by, direct = slice(0, cut), slice(cut, D)

    def by_way(target):
        return whole(via.at[:, by], fin_b.at[0, low_rows, by], via_s, out_r, target)

    def send_near(h):
        if h != 1 or not detour:
            send_end(0, h)
            return
        pl.when(s != 1)(lambda: send_end(0, h))

        @pl.when(s == 1)
        def _():
            remote(th.at[0, low_rows, by], via.at[:, by], out_s, via_r, dev(1, 0, 0))
            remote(
                th.at[0, low_rows, direct], fin_b.at[0, low_rows, direct],
                out_s, out_r, dev(-1, 0, 0),
            )

    def forward_via():
        if detour:
            @pl.when(s == 2)
            def _():
                whole(th.at[0, low_rows, by], via.at[:, by], out_s, via_r).wait_recv()
                by_way(dev(-2, 0, 0)).start()

    def forward_first(k, c):
        arrived(0, k, c)
        rows = rx_f[k, :, :, chunks[c]].astype(F32).reshape(G * C, -1)
        lanes = [rows[:, i : i + 128] for i in range(0, rows.shape[1], 128)]
        square = sum(lane * lane for lane in lanes)
        square_f[...] = square if c == 0 else square_f[...] + square
        scaled = (rows * gain_f[:, chunks[c]]).astype(BF16)
        for f in range(0, 2 * F, tile_f):
            hidden = dot(scaled, wi[chunks[c], f : f + tile_f])
            columns = slice(f, f + tile_f)
            sum_f[:, columns] = hidden if c == 0 else sum_f[:, columns] + hidden

    def forward_hidden():
        mean = jnp.sum(square_f[...], axis=-1, keepdims=True) * (1.0 / D)
        inverse = lax.rsqrt(mean + epsilon)
        for f in range(0, F, tile_f):
            gate = sum_f[:, f : f + tile_f] * inverse
            up = sum_f[:, F + f : F + f + tile_f] * inverse
            hidden_ref[:, f : f + tile_f] = (jax.nn.silu(gate) * up).astype(BF16)

    def forward_second(k, c):
        for d in range(chunks[c].start, chunks[c].stop, tile_d):
            columns = slice(d, d + tile_d)
            put_part(0, k, dot(hidden_ref[...], wo[:, columns]), columns)
        send_part(0, k, c)

    def forward_end(k, c):
        total = summed(0, k, c)
        moved = rx_f[k, 0, :, chunks[c]].astype(F32) + rg_f[k][:, :1] * total
        if k == 0:
            fin_f[0, :, chunks[c]] = moved.astype(BF16)
            return
        mv[k, :, chunks[c]] = moved.astype(BF16)
        remote(
            mv.at[k, :, chunks[c]], fin_f.at[k, :, chunks[c]],
            move_s.at[k - 1], move_r.at[k - 1], dev(0, -k, 0),
        )

    tile_f = tile_of(F, 256)
    with jax.named_scope("w_small"):
        for load in (load_gid, *load_small):
            load.wait()
    gather_f, scatter_f = placing(fid_ref[...], e, E, C, us_f.shape[1])
    gather_b, scatter_b = placing(gid_ref[...], e, E, C, us_b.shape[1])
    gather_f_rows, gather_b_rows = gather_f.astype(BF16), gather_b.astype(BF16)
    us_b[...] = scatter_b
    us_f[...] = scatter_f
    gates_b = jnp.sum(gather_b * ggate_ref[...], axis=1, keepdims=True)
    gates_f = jnp.sum(gather_f * fgate_ref[...], axis=1, keepdims=True)
    gs_f[...] = jnp.broadcast_to(gates_f, (T, gs_f.shape[2])).reshape(gs_f.shape)
    early = count // 2
    with jax.named_scope("w_x"):
        load_x.wait()
    for c in range(count):
        xs_f[:, :, chunks[c]] = (
            dot(gather_f_rows, x_ref[:, chunks[c]]).reshape(E, C, -1).astype(BF16)
        )
    arrivals = len(near) + 1 + (s + pipes - 1) // pipes

    def send_forward(order):
        for k, c in order:
            outgoing(0, k, c).start()

    far = [(k, c) for k in others for c in range(count)]
    own_rows = [(0, c) for c in range(count)]

    @pl.when(last)
    def _():
        pl.semaphore_wait(barrier, arrivals)
        send_forward(own_rows[-1:])

    with jax.named_scope("w_g"):
        load_g.wait()
    for c in range(count):
        rows = dot(gather_b_rows, g_ref[:, chunks[c]]).reshape(E, C, -1).astype(BF16)
        xs_b[:, :, chunks[c]] = rows
        rx_b[0, 0, :, chunks[c]] = rows[0]
    with jax.named_scope("w_bar"):
        pl.when(s != pipes - 1)(lambda: pl.semaphore_wait(barrier, arrivals))
    gain_copy = remote(gain_ref, gain_f, perm_s.at[2], perm_r.at[2], dev(1, 0, 0))
    remote(gs_f.at[0], rg_f.at[0], gate_s, gate_r, dev(1, 0, 0))
    perm_f = remote(us_f, ur_f, perm_s.at[0], perm_r.at[0], dev(1, 0, 0))

    greet(side_sem, beside)
    pl.when(s != pipes - 1)(lambda: send_forward(own_rows))
    for c in range(count):
        for k in others:
            outgoing(1, k, c).start()
    for j in range(1, G):
        same(1, j, xs_b.at[0]).start()
    pl.when(last)(lambda: greet(ready_sem, following))
    with jax.named_scope("w_saved"):
        load_saved.wait()
    srt[...] = dot(gather_b_rows, saved_ref[...]).reshape(E, C, D).astype(BF16)
    with stage("w_side"):
        pl.semaphore_wait(side_sem, len(beside))
    for k in others:
        remote(gs_f.at[k], rg_f.at[k], gate_s, gate_r, dev(1, k, 0))
    send_forward(far)
    pl.when(last)(lambda: send_forward(own_rows[:-1]))

    with jax.named_scope("w_wo"):
        load_wo.wait()
        load_acts.wait()
    with stage("b1_0"):
        for c in range(count):
            backward_first(0, c)
        backward_hidden(0)
    with jax.named_scope("w_wi"):
        load_wi.wait()

    def near_end():
        whole(us_b, ur_b, perm_s.at[1], perm_r.at[1], dev(-1, 0, 0)).start()
        for h in range(halves):
            send_near(h)

    def last_ends():
        for k in others:
            for h in range(1, halves):
                with stage(f"bend1_{h}"):
                    backward_end(k, h)
                    send_end(k, h)

    for c in range(count):
        with stage(f"b2_0_{c}"):
            backward_second(0, c)
        if 1 <= c <= early:
            for k in others:
                pass_on(1, k, c - 1)
    for c in range(early):
        with stage(f"b1_1a{c}"):
            backward_first(1, c)
        if c == 0:
            for k in others:
                for i in range(early, count - 1):
                    pass_on(1, k, i)
    for k in others:
        pass_on(1, k, count - 1)
    with stage("bend0"):
        for h in range(halves):
            backward_end(0, h)
    for k in others:
        with stage("b1_1b"):
            for c in range(early if k == 1 else 0, count):
                backward_first(k, c)
            backward_hidden(k)
        for c in range(count):
            with stage(f"b2_1_{c}"):
                backward_second(k, c)
            if k == 1 and c == min(2, count - 1):
                pl.when(s != 0)(near_end)
            if k == E - 1 and c >= early > 0:
                for other in others:
                    pass_on(0, other, c - early)
            if c >= 1:
                with stage(f"bret_{c - 1}"):
                    backward_return(k, c - 1)
        if k == E - 1:
            for other in others:
                for c in range(early, count - 1):
                    pass_on(0, other, c)
        with stage(f"bret_{count - 1}"):
            backward_return(k, count - 1)
        if k == E - 1:
            for other in others:
                pass_on(0, other, count - 1)
        for h in range(1, halves):
            for c in range(count):
                send_back(k, c, h)
    with jax.named_scope("w_gain"):
        gain_copy.wait_recv()
    with jax.named_scope("w_prev"):
        pl.when(first)(lambda: pl.semaphore_wait(ready_sem, 1))
        pl.when(first)(near_end)
    with jax.named_scope("w_gate"):
        whole(gs_f, rg_f, gate_s, gate_r).wait_recv()
    for k in others:
        for c in range(count):
            with stage(f"f1_1_{c}"):
                forward_first(k, c)
        with stage("fh_1"):
            forward_hidden()
        if k == 1:
            with jax.named_scope("w_via"):
                forward_via()
        for c in range(count):
            with stage(f"f2_1_{c}"):
                forward_second(k, c)
            if c == max(LAG, count - 2) or count == 1:
                with stage("bend1_0"):
                    backward_end(k, 0)
                    send_end(k, 0)
            if c >= LAG:
                with stage(f"fend_1_{c - LAG}"):
                    forward_end(k, c - LAG)
        if k == E - 1:
            with jax.named_scope("pass_0_0"):
                whole(xs_f.at[0], rx_f.at[0, 0], disp_s.at[0], row_r).wait_recv()
            for j in range(1, G):
                same(0, j, rx_f.at[0, 0]).start()
        for c in range(max(count - LAG, 0), count):
            with stage(f"fend_1_{c}"):
                forward_end(k, c)
    for c in range(count):
        with stage(f"f1_0_{c}"):
            forward_first(0, c)
        if c == early - 1:
            last_ends()
    with stage("fh_0"):
        forward_hidden()
    with stage("f2_0"):
        for c in range(count):
            forward_second(0, c)
    if early == 0:
        last_ends()
    with stage("fend0"):
        wait_near(0)
        for c in range(count):
            forward_end(0, c)

    with jax.named_scope("w_perm"):
        perm_f.wait_recv()
        whole(us_b, ur_b, perm_s.at[1], perm_r.at[1]).wait_recv()
    for k in others:
        with jax.named_scope("w_move"):
            whole(mv.at[k], fin_f.at[k], move_s.at[k - 1], move_r.at[k - 1]).wait_recv()
    with jax.named_scope("w_out"):
        whole(th, fin_b, out_s, out_r).wait_recv()
    with jax.named_scope("w_sends"):
        for b in range(2):
            rows = xs[b].at[pl.ds(b, E - b)]
            whole(rows, rows, disp_s.at[b], row_r).wait_send()
            for j in range(1, G):
                for sem in (relay_s, red_s):
                    whole(xs[b], xs[b], sem.at[b, j - 1], row_r).wait_send()
        for k in others:
            whole(pb.at[k], ret_b.at[k], ret_s.at[k - 1], ret_r.at[k - 1, 0]).wait_send()
            whole(mv.at[k], fin_f.at[k], move_s.at[k - 1], move_r.at[k - 1]).wait_send()
        whole(th, fin_b, out_s, out_r).wait_send()
        whole(gs_f, rg_f, gate_s, gate_r).wait_send()
        if detour:
            pl.when(s == 2)(lambda: by_way(dev(-2, 0, 0)).wait_send())
        for copy in (gain_copy, perm_f, whole(us_b, ur_b, perm_s.at[1], perm_r.at[1])):
            copy.wait_send()


UNSORT_STEPS = 2


def unsort(fin_f, fin_b, ur_f, ur_b, fout_hbm, gout_hbm, held, sems):
    T, D = fout_hbm.shape
    width = D // UNSORT_STEPS
    copies = []
    for i, (fin, ur, out) in enumerate(((fin_f, ur_f, fout_hbm), (fin_b, ur_b, gout_hbm))):
        for c in range(UNSORT_STEPS):
            columns = pl.ds(c * width, width)
            rows = fin[:, :, columns].astype(F32).reshape(T, width).astype(BF16)
            held[i, :, columns] = dot(ur[:, :T], rows).astype(BF16)
            copy = pltpu.make_async_copy(held.at[i, :, columns], out.at[:, columns], sems.at[i, c])
            copy.start()
            copies.append(copy)
    for copy in copies:
        copy.wait()


def on_device(
    dims,
    forward_in,
    forward_ids,
    forward_gates,
    grad_in,
    grad_ids,
    grad_gates,
    saved_input,
    saved_acts,
    norm_gain,
    weight_in,
    weight_out,
):
    pipes, E, G = dims
    T, D = forward_in.shape[1:]
    F = weight_out.shape[1]
    C = T // E
    padded = -(-T // 128) * 128
    DMA = pltpu.SemaphoreType.DMA
    rows = (E, C, D)
    vmem = pl.BlockSpec(memory_space=pltpu.VMEM)
    hbm = pl.BlockSpec(memory_space=pl.ANY)
    sorted_rows = jax.ShapeDtypeStruct(rows, BF16)
    order = jax.ShapeDtypeStruct((T, padded), BF16)
    halves, N = disp_rows(C), len(columns_of(D, C))
    arrived = pl.pallas_call(
        functools.partial(kernel, dims),
        out_shape=(pltpu.VMEM(rows, BF16), pltpu.VMEM(rows, BF16), pltpu.VMEM((T, padded), BF16), pltpu.VMEM((T, padded), BF16)),
        in_specs=[hbm] * 11,
        out_specs=(vmem, vmem, vmem, vmem),
        scratch_shapes=[
            pltpu.VMEM((1, T), jnp.int32), pltpu.VMEM((1, T), F32),
            pltpu.VMEM((1, T), jnp.int32), pltpu.VMEM((1, T), F32),
            pltpu.VMEM((1, D), F32),
            pltpu.VMEM((T, D), BF16), pltpu.VMEM((T, D), BF16), pltpu.VMEM((T, D), BF16),
            pltpu.VMEM((E * G, C, 2 * F), BF16),
            pltpu.VMEM((D, 2 * F), BF16),
            pltpu.VMEM((F, D), BF16),
            pltpu.VMEM((1, D), F32),
            pltpu.VMEM(rows, BF16), pltpu.VMEM(rows, BF16),
            pltpu.VMEM((E, G, C, D), BF16), pltpu.VMEM((E, G, C, D), BF16),
            pltpu.VMEM((E, C, 128), F32), pltpu.VMEM((E, C, 128), F32),
            pltpu.VMEM((T, padded), BF16), pltpu.VMEM((T, padded), BF16),
            pltpu.VMEM((E, G, C, D), BF16), pltpu.VMEM((E, G, C, D), BF16),
            pltpu.VMEM((E, G, C, D), BF16), pltpu.VMEM((E, G, C, D), BF16),
            pltpu.VMEM(rows, F32), pltpu.VMEM(rows, F32),
            pltpu.VMEM(rows, BF16), pltpu.VMEM(rows, BF16), pltpu.VMEM(rows, BF16),
            pltpu.VMEM(rows, BF16), pltpu.VMEM(rows, BF16),
            pltpu.VMEM((G * C, F), BF16),
            pltpu.VMEM((G * C, 2 * F), BF16),
            pltpu.VMEM((G * C, F), F32), pltpu.VMEM((G * C, 2 * F), F32),
            pltpu.VMEM((G * C, 2 * F), F32), pltpu.VMEM((G * C, 128), F32),
            pltpu.VMEM((C // halves, D), BF16),
            DMA((11,)), pltpu.SemaphoreType.REGULAR, pltpu.SemaphoreType.REGULAR, DMA, DMA,
            DMA((2,)), DMA((2, E - 1, N)), DMA, DMA,
            DMA((2, G - 1)), DMA((2, E - 1, G - 1, N)), DMA((3,)), DMA((3,)),
            DMA((2, G - 1)), DMA((2, E - 1, G - 1, N)), DMA((2, G - 1)),
            DMA, DMA((2, G - 1)),
            DMA((E - 1,)), DMA((E - 1,)), DMA, DMA,
            DMA((E - 1,)), DMA((E - 1, halves)),
        ],
        compiler_params=pltpu.CompilerParams(
            collective_id=0, has_side_effects=True, vmem_limit_bytes=40 * 2**20
        ),
    )(*[
        pltpu.with_memory_space_constraint(a, pltpu.HBM)
        for a in (
            forward_ids.reshape(1, T),
            forward_gates.reshape(1, T),
            grad_ids.reshape(1, T),
            grad_gates.reshape(1, T),
            norm_gain,
            forward_in[0],
            grad_in[0],
            saved_input[0],
            saved_acts.reshape(E * G, C, 2 * F),
            weight_in[0],
            weight_out[0],
        )
    ])
    out_shape = jax.ShapeDtypeStruct((T, D), BF16)
    fwd, grad = pl.pallas_call(
        unsort,
        out_shape=(out_shape, out_shape),
        in_specs=[vmem] * 4,
        out_specs=(hbm, hbm),
        scratch_shapes=[pltpu.VMEM((2, T, D), BF16), DMA((2, UNSORT_STEPS))],
        compiler_params=pltpu.CompilerParams(vmem_limit_bytes=8 * 2**20),
    )(*[pltpu.with_memory_space_constraint(a, pltpu.VMEM) for a in arrived])
    return fwd[None], grad[None]


def solution(mesh):
    sources = mesh.shape["expert"]
    G = min(4, sources // 2)
    dims = (mesh.shape["pipe"], sources // G, G)
    placed = (
        P("pipe", "expert", None),
        P("pipe", "expert", None),
        P("pipe", "expert", None),
        P("pipe", "expert", None),
        P("pipe", "expert", None),
        P("pipe", "expert", None),
        P("pipe", "expert", None),
        P("pipe", "expert", None, None),
        P("pipe", None),
        P("expert", None, None),
        P("expert", None, None),
    )
    return jax.shard_map(
        functools.partial(on_device, dims),
        mesh=mesh,
        in_specs=placed,
        out_specs=(P("pipe", "expert", None), P("pipe", "expert", None)),
        check_vma=False,
    )
```
